32 devices in a mesh: dp: 8 (over y, x, core), tensor: 4 (over z).
Axes of the slice: x: 2, y: 2, z: 4, core: 2. Of those that a mesh axis runs over, the one named last changes fastest.
Arguments:
- tokens: bfloat16 [1024, 8, 1280], P('tensor', 'dp'), may hold values from -6 to 6
- cotangent: bfloat16 [1024, 8, 1280], P('tensor', 'dp'), may hold values from -6 to 6
- qkv_weight: float32 [3, 1280, 1280], P(None, 'dp', 'tensor'), may hold values from -0.15625 to 0.15625
- out_weight: float32 [1280, 1280], P('tensor', 'dp'), may hold values from -1.25 to 1.25
- expand_weight: float32 [1280, 5120], P('dp', 'tensor'), may hold values from -0.15625 to 0.15625
- reduce_weight: float32 [5120, 1280], P('tensor', 'dp'), may hold values from -0.078125 to 0.078125
- gains_biases: float32 [15360], P(('dp', 'tensor')), may hold values from -1 to 2, as said below
- rel_tables: float32 [2, 63, 80], replicated, may hold values from -1.5 to 1.5
- qkv_moment: float32 [3, 1280, 1280], P(None, 'dp', 'tensor'), may hold values from -192 to 192
- out_moment: float32 [1280, 1280], P('tensor', 'dp'), may hold values from -192 to 192
- expand_moment: float32 [1280, 5120], P('dp', 'tensor'), may hold values from -192 to 192
- reduce_moment: float32 [5120, 1280], P('tensor', 'dp'), may hold values from -192 to 192
- gains_moment: float32 [15360], P(('dp', 'tensor')), may hold values from -640 to 640
- rel_moment: float32 [2, 63, 80], replicated, may hold values from -1536 to 1536
- qkv_average: float32 [3, 1280, 1280], P(None, 'dp', 'tensor'), may hold values from -0.15625 to 0.15625
- out_average: float32 [1280, 1280], P('tensor', 'dp'), may hold values from -1.25 to 1.25
- expand_average: float32 [1280, 5120], P('dp', 'tensor'), may hold values from -0.15625 to 0.15625
- reduce_average: float32 [5120, 1280], P('tensor', 'dp'), may hold values from -0.078125 to 0.078125
- gains_average: float32 [15360], P(('dp', 'tensor')), may hold values from 0.1 to 1.9
- rel_average: float32 [2, 63, 80], replicated, may hold values from -1.5 to 1.5
Outputs:
- block_out: bfloat16 [1024, 8, 1280], P('tensor', 'dp')
- token_grad: float32 [1024, 8, 1280], P('tensor', 'dp')
- qkv_grad: float32 [3, 1280, 1280], P(None, 'dp', 'tensor')
- out_grad: float32 [1280, 1280], P('tensor', 'dp')
- expand_grad: float32 [1280, 5120], P('dp', 'tensor')
- reduce_grad: float32 [5120, 1280], P('tensor', 'dp')
- gains_grad: float32 [15360], P(('dp', 'tensor'))
- rel_grad: float32 [2, 63, 80], replicated
- new_qkv: float32 [3, 1280, 1280], P(None, 'dp', 'tensor')
- new_out: float32 [1280, 1280], P('tensor', 'dp')
- new_expand: float32 [1280, 5120], P('dp', 'tensor')
- new_reduce: float32 [5120, 1280], P('tensor', 'dp')
- new_gains: float32 [15360], P(('dp', 'tensor'))
- new_rel: float32 [2, 63, 80], replicated
- moment_qkv: float32 [3, 1280, 1280], P(None, 'dp', 'tensor')
- moment_out: float32 [1280, 1280], P('tensor', 'dp')
- moment_expand: float32 [1280, 5120], P('dp', 'tensor')
- moment_reduce: float32 [5120, 1280], P('tensor', 'dp')
- moment_gains: float32 [15360], P(('dp', 'tensor'))
- moment_rel: float32 [2, 63, 80], replicated
- average_qkv: float32 [3, 1280, 1280], P(None, 'dp', 'tensor')
- average_out: float32 [1280, 1280], P('tensor', 'dp')
- average_expand: float32 [1280, 5120], P('dp', 'tensor')
- average_reduce: float32 [5120, 1280], P('tensor', 'dp')
- average_gains: float32 [15360], P(('dp', 'tensor'))
- average_rel: float32 [2, 63, 80], replicated
The draws below stay inside these ranges and needn't reach their ends.
Inputs may be any that keep to these rules, and one draw needn't show every extreme that they name: `gains_biases`: the two norm gains lie between 0.5 and 1.5.
All inputs are finite; a program needn't handle non-finite values.
Results may differ from the reference program's by a relative error of at most 0.015.
The reference program's roundings to bfloat16 on the way count: a program that leaves them out, or rounds other values in their place, can miss the bound.
Values may be sent and summed in bfloat16 or wider, within the bound.
A program may use at most 192 MiB of HBM per device.

```python
import math
import jax
import jax.numpy as jnp
from jax import lax

D = 1280
HD = 80
FF = 5120
GRID = 32
IMAGES = 8
SEQ = 1024
OFFSETS = 63
VEC = 15360


def draw_gains_biases(key, part):
    normal_part = jax.random.normal(jax.random.fold_in(key, 1), (8 * D + FF,), jnp.float32)
    spread_part = jax.random.uniform(jax.random.fold_in(key, 2), (8 * D + FF,), jnp.float32, 0.5, 1.5)
    position = jnp.arange(8 * D + FF)
    section = position // D
    is_gain = (section == 0) | (section == 5)
    return jnp.where(is_gain, spread_part, 0.25 * jnp.clip(normal_part, -4.0, 4.0))


def block_scale(stream_key, dims, pieces, least, top_value):
    gain, own = 1.0, jax.random.fold_in(stream_key, 6)
    for dim, parts in pieces:
        steps = jnp.exp(jax.random.uniform(jax.random.fold_in(own, dim), (parts,), jnp.float32, least / len(pieces), top_value / len(pieces)))
        gain = gain * jnp.repeat(steps, dims[dim] // parts).reshape([-1 if axis == dim else 1 for axis in range(len(dims))])
    return gain


def bell_draw(key, dims, spread, limit, split=(), dtype=jnp.bfloat16):
    result = spread * jax.random.normal(key, dims, jnp.float32)
    if split:
        result = result * block_scale(key, dims, split, -0.22, 0.18)
    return jnp.clip(result, -limit, limit).astype(dtype)


def setup_inputs(seed: int = 0) -> dict:
    splits = jax.random.split(jax.random.key(seed), 21)
    tokens = bell_draw(splits[0], (SEQ, IMAGES, D), 1.0, 6.0, ((0, 4), (1, 8)))
    cotangent = bell_draw(splits[1], (SEQ, IMAGES, D), 1.0, 6.0, ((0, 4), (1, 8)))
    qkv_weight = bell_draw(splits[2], (3, D, D), D ** -0.5, 0.15625, ((1, 8), (2, 4)), jnp.float32)
    out_weight = bell_draw(splits[3], (D, D), (D * 16 // (GRID * GRID)) ** -0.5, 1.25, ((0, 4), (1, 8)), jnp.float32)
    expand_weight = bell_draw(splits[4], (D, FF), D ** -0.5, 0.15625, ((0, 8), (1, 4)), jnp.float32)
    reduce_weight = bell_draw(splits[5], (FF, D), FF ** -0.5, 0.078125, ((0, 4), (1, 8)), jnp.float32)
    gains_biases = draw_gains_biases(jax.random.fold_in(splits[20], 71), 0)
    rel_tables = bell_draw(splits[7], (2, OFFSETS, HD), 0.1, 1.5, (), jnp.float32)
    qkv_moment = bell_draw(splits[8], (3, D, D), 30.0, 192.0, ((1, 8), (2, 4)), jnp.float32)
    out_moment = bell_draw(splits[9], (D, D), 30.0, 192.0, ((0, 4), (1, 8)), jnp.float32)
    expand_moment = bell_draw(splits[10], (D, FF), 30.0, 192.0, ((0, 8), (1, 4)), jnp.float32)
    reduce_moment = bell_draw(splits[11], (FF, D), 30.0, 192.0, ((0, 4), (1, 8)), jnp.float32)
    gains_moment = bell_draw(splits[12], (VEC,), 100.0, 640.0, ((0, 32),), jnp.float32)
    rel_moment = bell_draw(splits[13], (2, OFFSETS, HD), (GRID * GRID * (IMAGES + 24) // 128), 1536.0, (), jnp.float32)
    qkv_average = bell_draw(splits[14], (3, D, D), D ** -0.5, 0.15625, ((1, 8), (2, 4)), jnp.float32)
    out_average = bell_draw(splits[15], (D, D), (D * 16 // (GRID * GRID)) ** -0.5, 1.25, ((0, 4), (1, 8)), jnp.float32)
    expand_average = bell_draw(splits[16], (D, FF), D ** -0.5, 0.15625, ((0, 8), (1, 4)), jnp.float32)
    reduce_average = bell_draw(splits[17], (FF, D), FF ** -0.5, 0.078125, ((0, 4), (1, 8)), jnp.float32)
    gains_average = jnp.clip(1.0 + 0.18 * jax.random.normal(splits[18], (VEC,), jnp.float32), 0.1, 1.9)
    rel_average = bell_draw(splits[19], (2, OFFSETS, HD), 0.1, 1.5, (), jnp.float32)
    return {"tokens": tokens, "cotangent": cotangent, "qkv_weight": qkv_weight, "out_weight": out_weight, "expand_weight": expand_weight, "reduce_weight": reduce_weight, "gains_biases": gains_biases, "rel_tables": rel_tables, "qkv_moment": qkv_moment, "out_moment": out_moment, "expand_moment": expand_moment, "reduce_moment": reduce_moment, "gains_moment": gains_moment, "rel_moment": rel_moment, "qkv_average": qkv_average, "out_average": out_average, "expand_average": expand_average, "reduce_average": reduce_average, "gains_average": gains_average, "rel_average": rel_average}


PRECISE = lax.Precision.HIGHEST
EPSILON = 1e-06
MOMENTUM = 0.5
AVERAGING = 0.5
RATE_MAIN = 0.0003
RATE_TABLES = 0.01

@jax.custom_vjp
def low(v):
    return lax.optimization_barrier(v.astype(jnp.bfloat16)).astype(jnp.float32)

@jax.custom_vjp
def low_back(v):
    return v

def low_keep(v):
    return (low(v), None)

def low_pass(kept, grad):
    return (grad,)

def back_keep(v):
    return (v, None)

def back_low(kept, grad):
    return (low(grad),)
low.defvjp(low_keep, low_pass)
low_back.defvjp(back_keep, back_low)

def matmul(left, right):
    return jnp.dot(left, right, precision=PRECISE, preferred_element_type=jnp.float32)

def offset_table(grid_side):
    table_shape = (grid_side, grid_side, 2 * grid_side - 1)
    first_axis = lax.broadcasted_iota(jnp.int32, table_shape, 0)
    second_axis = lax.broadcasted_iota(jnp.int32, table_shape, 1)
    third_axis = lax.broadcasted_iota(jnp.int32, table_shape, 2)
    return (third_axis == first_axis - second_axis + grid_side - 1).astype(jnp.float32)

def layer_norm(values, gain_row, shift_row):
    center = values - lax.optimization_barrier(jnp.mean(values, axis=-1, keepdims=True))
    inverse = lax.rsqrt(lax.optimization_barrier(jnp.mean(center * center, axis=-1, keepdims=True)) + EPSILON)
    return center * inverse * gain_row + shift_row

def attend(query_rows, key_rows, value_rows, rel_rows, rel_cols):
    seq_length, head_count, head_size = query_rows.shape
    grid_side = rel_rows.shape[0]
    shaped = query_rows.reshape(grid_side, grid_side, head_count, head_size)
    row_bias = low_back(jnp.einsum('abhc,akc->habk', shaped, rel_rows, precision=PRECISE))
    col_bias = low_back(jnp.einsum('abhc,bkc->habk', shaped, rel_cols, precision=PRECISE))
    dot_scores = jnp.einsum('qhc,khc->hqk', query_rows, key_rows, precision=PRECISE) * head_size ** (-0.5)
    scores = dot_scores.reshape(head_count, grid_side, grid_side, grid_side, grid_side)
    scores = scores + row_bias[..., :, None] + col_bias[..., None, :]
    scores = low_back(scores.reshape(head_count, seq_length, seq_length))
    probabilities = low(jax.nn.softmax(scores, axis=-1))
    return jnp.einsum('hqk,khc->qhc', probabilities, value_rows, precision=PRECISE)

def run_block(qkv_weight, out_weight, expand_weight, reduce_weight, gains_biases, rel_tables, token_values):
    seq_length, images, model_width = token_values.shape
    head_size = rel_tables.shape[2]
    head_count = model_width // head_size
    grid_side = (rel_tables.shape[1] + 1) // 2
    group_size = math.gcd(images, 4)
    qkv_low = low(qkv_weight)
    out_low = low(out_weight)
    expand_low = low(expand_weight)
    reduce_low = low(reduce_weight)
    offsets = offset_table(grid_side)
    rel_low = low(rel_tables)
    rel_rows = jnp.einsum('akr,rc->akc', offsets, rel_low[0], precision=PRECISE)
    rel_cols = jnp.einsum('akr,rc->akc', offsets, rel_low[1], precision=PRECISE)

    def segment(position):
        return gains_biases[position * model_width:(position + 1) * model_width]
    expand_bias = gains_biases[8 * model_width:]

    def split_heads(row_values, members):
        return row_values.reshape(seq_length, members, head_count, head_size).transpose(1, 0, 2, 3)

    def one_image(triple):
        return attend(triple[0], triple[1], triple[2], rel_rows, rel_cols)

    def group_block(values_group):
        members = values_group.shape[1]
        token_rows = values_group.reshape(seq_length * members, model_width)
        normed_one = low(layer_norm(token_rows, segment(0), segment(1)))
        query_rows = low_back(low(matmul(normed_one, qkv_low[0]) + segment(2)))
        key_rows = low_back(low(matmul(normed_one, qkv_low[1])))
        value_rows = low_back(low(matmul(normed_one, qkv_low[2]) + segment(3)))
        contexts = lax.map(jax.checkpoint(one_image), (split_heads(query_rows, members), split_heads(key_rows, members), split_heads(value_rows, members)))
        context_rows = contexts.transpose(1, 0, 2, 3).reshape(seq_length * members, model_width)
        context_rows = low_back(low(context_rows))
        attn_out = low_back(matmul(context_rows, out_low) + segment(4))
        mid_rows = token_rows + attn_out
        normed_two = low(layer_norm(mid_rows, segment(5), segment(6)))
        hidden_pre = low_back(matmul(normed_two, expand_low) + expand_bias)
        hidden_act = low(jax.nn.gelu(hidden_pre, approximate=False))
        mlp_out = low_back(matmul(hidden_act, reduce_low) + segment(7))
        return (mid_rows + mlp_out).reshape(seq_length, members, model_width)
    grouped = token_values.reshape(seq_length, images // group_size, group_size, model_width).transpose(1, 0, 2, 3)
    outputs = lax.map(jax.checkpoint(group_block), grouped)
    return outputs.transpose(1, 0, 2, 3).reshape(seq_length, images, model_width)

def advance(weight, moment, average, gradient, rate):
    new_moment = MOMENTUM * moment + gradient
    new_weight = weight - rate * (gradient + MOMENTUM * new_moment)
    new_average = AVERAGING * average + (1.0 - AVERAGING) * new_weight
    return (new_weight, new_moment, new_average)

def reference(tokens, cotangent, qkv_weight, out_weight, expand_weight, reduce_weight, gains_biases, rel_tables, qkv_moment, out_moment, expand_moment, reduce_moment, gains_moment, rel_moment, qkv_average, out_average, expand_average, reduce_average, gains_average, rel_average):
    block_value, pullback = jax.vjp(run_block, qkv_weight, out_weight, expand_weight, reduce_weight, gains_biases, rel_tables, tokens.astype(jnp.float32))
    grad_qkv, grad_out, grad_expand, grad_reduce, grad_gains, grad_rel, grad_tokens = pullback(cotangent.astype(jnp.float32))
    new_qkv, moment_qkv, average_qkv = advance(qkv_weight, qkv_moment, qkv_average, grad_qkv, RATE_MAIN)
    new_out, moment_out, average_out = advance(out_weight, out_moment, out_average, grad_out, RATE_MAIN)
    new_expand, moment_expand, average_expand = advance(expand_weight, expand_moment, expand_average, grad_expand, RATE_MAIN)
    new_reduce, moment_reduce, average_reduce = advance(reduce_weight, reduce_moment, reduce_average, grad_reduce, RATE_MAIN)
    new_gains, moment_gains, average_gains = advance(gains_biases, gains_moment, gains_average, grad_gains, RATE_MAIN)
    new_rel, moment_rel, average_rel = advance(rel_tables, rel_moment, rel_average, grad_rel, RATE_TABLES)
    return (block_value.astype(jnp.bfloat16), grad_tokens, grad_qkv, grad_out, grad_expand, grad_reduce, grad_gains, grad_rel, new_qkv, new_out, new_expand, new_reduce, new_gains, new_rel, moment_qkv, moment_out, moment_expand, moment_reduce, moment_gains, moment_rel, average_qkv, average_out, average_expand, average_reduce, average_gains, average_rel)
```

```python
import functools
import jax
import jax.numpy as jnp
from jax import lax
from jax.experimental import pallas as pl
from jax.experimental.pallas import tpu as pltpu
from jax.sharding import PartitionSpec as P

EPSILON = 1e-06
MOMENTUM = 0.5
AVERAGING = 0.5
RATE_MAIN = 0.0003
RATE_TABLES = 0.01
NARROW = jnp.bfloat16
SINGLE = jnp.float32


def normalize(values, gain_row, shift_row):
    center = values - jnp.mean(values, axis=-1, keepdims=True)
    inverse = lax.rsqrt(jnp.mean(center * center, axis=-1, keepdims=True) + EPSILON)
    scaled = center * inverse
    return (scaled * gain_row + shift_row, scaled, inverse)


def normalize_back(grad_output, scaled, inverse, gain_row):
    grad_scaled = grad_output * gain_row
    mean_plain = jnp.mean(grad_scaled, axis=-1, keepdims=True)
    mean_cross = jnp.mean(grad_scaled * scaled, axis=-1, keepdims=True)
    grad_values = inverse * (grad_scaled - mean_plain - scaled * mean_cross)
    return (grad_values, jnp.sum(grad_output * scaled, axis=0), jnp.sum(grad_output, axis=0))


def gelu_slope(values):
    cumulative = 0.5 * (1.0 + lax.erf(values * 0.7071067811865476))
    density = 0.3989422804014327 * jnp.exp(-0.5 * values * values)
    return cumulative + values * density


def contract_rows(left_side, right_side):
    return lax.dot_general(
        left_side, right_side, (((0,), (0,)), ((), ())), preferred_element_type=SINGLE
    )


def contract_cols(left_side, right_side):
    return lax.dot_general(
        left_side, right_side, (((1,), (1,)), ((), ())), preferred_element_type=SINGLE
    )


def dot_nt(left, right):
    return lax.dot_general(left, right, (((1,), (1,)), ((), ())), preferred_element_type=SINGLE)


def dot_tn(left, right):
    return lax.dot_general(left, right, (((0,), (0,)), ((), ())), preferred_element_type=SINGLE)


def dot_nn(left, right):
    return lax.dot_general(left, right, (((1,), (0,)), ((), ())), preferred_element_type=SINGLE)


def forward_kernel(
    heads, size, grid_side, block, qkv_ref, table_ref, hot_ref,
    out_ref, bias_ref, lse_ref, query_ext, key_ext, bias_wide, context_t,
):
    seq = qkv_ref.shape[0]
    width = heads * size
    scale = size ** (-0.5)
    lane = lax.broadcasted_iota(jnp.int32, (grid_side, 128), 1)
    query_ext[:, 0:128] = jnp.zeros((seq, 128), NARROW)
    key_ext[:, 0:128] = jnp.zeros((seq, 128), NARROW)
    key_ext[:, 128:256] = hot_ref[...]
    for head in range(heads):
        low = head * size
        query = qkv_ref[:, low : low + size]
        value = qkv_ref[:, 2 * width + low : 2 * width + low + size]
        query_ext[:, 0:size] = query
        key_ext[:, 0:size] = qkv_ref[:, width + low : width + low + size]
        bias_wide[...] = dot_nt(query, table_ref[...])
        for row in range(grid_side):
            rows = pl.ds(row * grid_side, grid_side)
            group = bias_wide[rows, :]
            part_row = pltpu.roll(group, (128 - grid_side + 1 + row) % 128, 1)
            part_col = pltpu.roll(group, 65 - 32 + grid_side, 1, stride=1, stride_axis=0)
            both = jnp.where(
                lane < grid_side, part_row, jnp.where(lane < 2 * grid_side, part_col, 0.0)
            ) * (size ** 0.5)
            high = both.astype(NARROW).astype(SINGLE)
            rest = pltpu.roll(both - high, 64, 1)
            mixed = jnp.where(lane < 64, high, rest).astype(NARROW)
            query_ext[rows, 128:256] = mixed
        bias_ref[head] = query_ext[:, 128:256]
        for start in range(0, seq, block):
            scores = dot_nt(key_ext[...], query_ext[start : start + block, :])
            highest = jnp.max(scores, axis=0, keepdims=True)
            powers = jnp.exp((scores - highest) * scale)
            total = jnp.sum(powers, axis=0, keepdims=True)
            weights = (powers * (1.0 / total)).astype(NARROW)
            lse_ref[head, :, start : start + block] = highest * scale + jnp.log(total)
            context_t[low : low + size, start : start + block] = dot_tn(value, weights)
    out_ref[...] = context_t[...].T.astype(NARROW)


def backward_kernel(
    heads, size, grid_side, block, qkv_ref, grad_ref, bias_ref, lse_ref, table_ref, hot_ref, rev_ref,
    out_ref, rel_ref, query_ext, key_ext, key_rev, spread, grad_keys, grad_values, grad_query,
):
    seq = qkv_ref.shape[0]
    width = heads * size
    scale = size ** (-0.5)
    lane = lax.broadcasted_iota(jnp.int32, (grid_side, 128), 1)
    query_ext[:, 0:128] = jnp.zeros((seq, 128), NARROW)
    key_ext[:, 0:128] = jnp.zeros((seq, 128), NARROW)
    key_ext[:, 128:256] = hot_ref[...]
    key_rev[:, 0:128] = jnp.zeros((seq, 128), NARROW)
    key_rev[:, 128:256] = rev_ref[...]
    rel_total = jnp.zeros(rel_ref.shape, SINGLE)
    for head in range(heads):
        low = head * size
        query = qkv_ref[:, low : low + size]
        key = qkv_ref[:, width + low : width + low + size]
        value = qkv_ref[:, 2 * width + low : 2 * width + low + size]
        grad = grad_ref[:, low : low + size]
        query_ext[:, 0:size] = query
        query_ext[:, 128:256] = bias_ref[head]
        key_ext[:, 0:size] = key
        key_rev[:, 0:size] = key
        for start in range(0, seq, block):
            part = slice(start, start + block)
            scores = dot_nt(key_ext[...], query_ext[part, :])
            soft = jnp.exp(scores * scale - lse_ref[head, :, part])
            grad_part = grad[part]
            grad_soft = dot_nt(value, grad_part)
            inner = jnp.sum(soft * grad_soft, axis=0, keepdims=True)
            grad_scores = (soft * (grad_soft - inner)).astype(NARROW)
            add_values = dot_nn(soft.astype(NARROW), grad_part)
            add_keys = dot_nn(grad_scores, query[part])
            if start == 0:
                grad_values[...] = add_values
                grad_keys[...] = add_keys
            else:
                grad_values[...] += add_values
                grad_keys[...] += add_keys
            turned = dot_tn(key_rev[...], grad_scores).T
            grad_query[part, :] = turned[:, 0:128]
            sums = turned[:, 128:256].astype(NARROW).astype(SINGLE)
            for inside in range(block // grid_side):
                row = start // grid_side + inside
                group = sums[inside * grid_side : (inside + 1) * grid_side]
                part_row = jnp.where(lane < grid_side, group, 0.0)
                part_col = jnp.where((lane >= grid_side) & (lane < 2 * grid_side), group, 0.0)
                if row:
                    part_row = pltpu.roll(part_row, row, 1)
                part_col = pltpu.roll(part_col, 64 - grid_side, 1, stride=1, stride_axis=0)
                spread[row * grid_side : (row + 1) * grid_side, :] = (part_row + part_col).astype(NARROW)
        total_query = grad_query[:, 0:size] * scale + dot_nn(spread[...], table_ref[...])
        out_ref[:, low : low + size] = total_query.astype(NARROW)
        out_ref[:, width + low : width + low + size] = (grad_keys[...] * scale).astype(NARROW)
        out_ref[:, 2 * width + low : 2 * width + low + size] = grad_values[...].astype(NARROW)
        rel_total = rel_total + dot_tn(spread[...], query)
    rel_ref[...] = rel_total


def attention_tables(rel_low, grid_side):
    offsets = rel_low.shape[1]
    pad = ((0, 0), (0, 64 - offsets), (0, 0))
    plain = jnp.pad(rel_low, pad).reshape(128, -1)
    turned = jnp.pad(rel_low[:, ::-1], pad).reshape(128, -1)
    seq = grid_side * grid_side
    token = lax.broadcasted_iota(jnp.int32, (seq, 128), 0)
    lane = lax.broadcasted_iota(jnp.int32, (seq, 128), 1)
    inside = lane % 64
    row, col = (token // grid_side, token % grid_side)
    hot = jnp.where(inside < grid_side, inside == row, inside - grid_side == col)
    hot = (hot & (inside < 2 * grid_side)).astype(NARROW)
    back = jnp.where(lane < grid_side, grid_side - 1 - lane == row, 2 * grid_side - 1 - lane == col)
    back = (back & (lane < 2 * grid_side)).astype(NARROW)
    return plain, turned, hot, back


def whole_vmem(count):
    return [pl.BlockSpec(memory_space=pltpu.VMEM)] * count


def attend_forward(qkv_rows, turned, hot, heads, size, grid_side):
    seq = qkv_rows.shape[0]
    block = min(256, seq)
    return pl.pallas_call(
        functools.partial(forward_kernel, heads, size, grid_side, block),
        out_shape=(
            jax.ShapeDtypeStruct((seq, heads * size), NARROW),
            jax.ShapeDtypeStruct((heads, seq, 128), NARROW),
            jax.ShapeDtypeStruct((heads, 1, seq), SINGLE),
        ),
        in_specs=whole_vmem(3),
        out_specs=tuple(whole_vmem(3)),
        scratch_shapes=[
            pltpu.VMEM((seq, 256), NARROW),
            pltpu.VMEM((seq, 256), NARROW),
            pltpu.VMEM((seq, 128), SINGLE),
            pltpu.VMEM((heads * size, seq), SINGLE),
        ],
        compiler_params=pltpu.CompilerParams(vmem_limit_bytes=40 << 20),
        name="attend_forward",
    )(qkv_rows, turned, hot)


def attend_backward(qkv_rows, grad_rows, bias, lse, plain, hot, back, heads, size, grid_side):
    seq = qkv_rows.shape[0]
    block = min(256, seq)
    return pl.pallas_call(
        functools.partial(backward_kernel, heads, size, grid_side, block),
        out_shape=(
            jax.ShapeDtypeStruct((seq, 3 * heads * size), NARROW),
            jax.ShapeDtypeStruct((128, size), SINGLE),
        ),
        in_specs=whole_vmem(7),
        out_specs=tuple(whole_vmem(2)),
        scratch_shapes=[
            pltpu.VMEM((seq, 256), NARROW),
            pltpu.VMEM((seq, 256), NARROW),
            pltpu.VMEM((seq, 256), NARROW),
            pltpu.VMEM((seq, 128), NARROW),
            pltpu.VMEM((seq, size), SINGLE),
            pltpu.VMEM((seq, size), SINGLE),
            pltpu.VMEM((seq, 128), SINGLE),
        ],
        compiler_params=pltpu.CompilerParams(vmem_limit_bytes=48 << 20),
        name="attend_backward",
    )(qkv_rows, grad_rows, bias, lse, plain, hot, back)


TILE = 1024


def as_tiles(vector):
    return jnp.pad(vector, (0, TILE - vector.shape[0])).reshape(8, 128)


def advance(weight, moment, average, gradient, rate_value):
    new_moment = MOMENTUM * moment + gradient
    new_weight = weight - rate_value * (gradient + MOMENTUM * new_moment)
    new_average = AVERAGING * average + (1.0 - AVERAGING) * new_weight
    return (new_weight, new_moment, new_average)


def local(
    tokens,
    cotangent,
    qkv_weight,
    out_weight,
    expand_weight,
    reduce_weight,
    gains_biases,
    rel_tables,
    qkv_moment,
    out_moment,
    expand_moment,
    reduce_moment,
    gains_moment,
    rel_moment,
    qkv_average,
    out_average,
    expand_average,
    reduce_average,
    gains_average,
    rel_average,
):
    local_seq, local_images, model_width = tokens.shape
    tensor_count = lax.axis_size("tensor")
    tensor_index = lax.axis_index("tensor")
    local_rows = local_seq * local_images
    seq_length = local_seq * tensor_count
    head_width = qkv_weight.shape[2]
    hidden_width = expand_weight.shape[1]
    head_size = rel_tables.shape[2]
    grid_side = (rel_tables.shape[1] + 1) // 2
    qkv_full, out_full, expand_full, reduce_full = (
        lax.all_gather(qkv_weight.astype(NARROW), "dp", axis=1, tiled=True),
        lax.all_gather(out_weight.astype(NARROW), "dp", axis=1, tiled=True),
        lax.all_gather(expand_weight.astype(NARROW), "dp", axis=0, tiled=True),
        lax.all_gather(reduce_weight.astype(NARROW), "dp", axis=1, tiled=True),
    )
    qkv_joined = qkv_full.transpose(1, 0, 2).reshape(model_width, 3 * head_width)
    piece = gains_biases.shape[0]
    params_all = lax.all_gather(
        as_tiles(gains_biases), ("dp", "tensor"), axis=0, tiled=False
    ).reshape(-1, TILE)[:, :piece].reshape(-1)

    def segment(position):
        return params_all[position * model_width : (position + 1) * model_width]

    query_bias = lax.dynamic_slice_in_dim(
        params_all, 2 * model_width + tensor_index * head_width, head_width
    )
    value_bias = lax.dynamic_slice_in_dim(
        params_all, 3 * model_width + tensor_index * head_width, head_width
    )
    heads = head_width // head_size
    plain, turned, hot, back = attention_tables(rel_tables.astype(NARROW), grid_side)
    token_rows = tokens.reshape(local_rows, model_width).astype(SINGLE)
    normed_one, scaled_one, inverse_one = normalize(token_rows, segment(0), segment(1))
    gathered_one = lax.all_gather(normed_one.astype(NARROW), "tensor", axis=0, tiled=True)
    projected = jnp.dot(gathered_one, qkv_joined, preferred_element_type=SINGLE)
    qkv_bias = jnp.concatenate([query_bias, jnp.zeros((head_width,), SINGLE), value_bias])
    qkv_rows = (projected + qkv_bias).astype(NARROW)
    context_rows, bias_wide, logsums = attend_forward(
        qkv_rows, turned, hot, heads, head_size, grid_side
    )
    mid_rows = token_rows + (
        lax.psum_scatter(
            jnp.dot(context_rows, out_full, preferred_element_type=SINGLE).astype(NARROW),
            "tensor",
            scatter_dimension=0,
            tiled=True,
        ).astype(SINGLE)
        + segment(4)
    )
    normed_two, scaled_two, inverse_two = normalize(mid_rows, segment(5), segment(6))
    normed_two_low = normed_two.astype(NARROW)
    expand_bias = lax.dynamic_slice_in_dim(
        params_all, 8 * model_width + tensor_index * hidden_width, hidden_width
    )
    gathered_two = lax.all_gather(normed_two_low, "tensor", axis=0, tiled=True)
    hidden_pre = jnp.dot(gathered_two, expand_full, preferred_element_type=SINGLE) + expand_bias
    hidden_low = jax.nn.gelu(hidden_pre, approximate=False).astype(NARROW)
    mlp_sum = lax.psum_scatter(
        jnp.dot(hidden_low, reduce_full, preferred_element_type=SINGLE).astype(jnp.bfloat16),
        "tensor",
        scatter_dimension=0,
        tiled=True,
    ).astype(jnp.float32)
    block_rows = mid_rows + (mlp_sum + segment(7))
    block_out = block_rows.astype(NARROW).reshape(tokens.shape)
    cotangent_rows = cotangent.reshape(local_rows, model_width)
    grad_block = cotangent_rows.astype(SINGLE)
    grad_reduce_bias = jnp.sum(grad_block, axis=0)
    shard_rows = lax.all_gather(cotangent_rows, "tensor", axis=0, tiled=True)
    part_hidden = contract_cols(shard_rows, reduce_full)
    grad_hidden = part_hidden
    grad_hidden, grad_reduce = (grad_hidden, contract_rows(hidden_low, shard_rows))
    grad_pre = (grad_hidden * gelu_slope(hidden_pre)).astype(NARROW)
    grad_expand = contract_rows(gathered_two, grad_pre)
    grad_expand_bias = jnp.sum(grad_pre, axis=0, dtype=SINGLE)
    expand_bias_full = lax.dynamic_update_slice_in_dim(
        jnp.zeros((hidden_width * tensor_count,), SINGLE),
        grad_expand_bias,
        tensor_index * hidden_width,
        0,
    )
    grad_normed_two = lax.psum_scatter(
        contract_cols(grad_pre, expand_full).astype(jnp.bfloat16),
        "tensor",
        scatter_dimension=0,
        tiled=True,
    ).astype(jnp.float32)
    grad_mid_norm, grad_gain_two, grad_shift_two = normalize_back(
        grad_normed_two, scaled_two, inverse_two, segment(5)
    )
    grad_mid = grad_block + grad_mid_norm
    grad_attn_low = grad_mid.astype(NARROW)
    grad_out_bias = jnp.sum(grad_attn_low, axis=0, dtype=SINGLE)
    shard_rows = lax.all_gather(grad_attn_low, "tensor", axis=0, tiled=True)
    part_context = contract_cols(shard_rows, out_full)
    grad_context = part_context
    grad_context, grad_out = (grad_context, contract_rows(context_rows, shard_rows))
    grad_qkv_rows, grad_tables = attend_backward(
        qkv_rows, grad_context.astype(NARROW), bias_wide, logsums, plain, hot, back,
        heads, head_size, grid_side,
    )
    grad_query_rows = grad_qkv_rows[:, :head_width]
    grad_value_rows = grad_qkv_rows[:, 2 * head_width :]
    grad_query_bias = jnp.sum(grad_query_rows, axis=0, dtype=SINGLE)
    grad_value_bias = jnp.sum(grad_value_rows, axis=0, dtype=SINGLE)
    grad_qkv = (
        contract_rows(gathered_one, grad_qkv_rows)
        .reshape(model_width, 3, head_width)
        .transpose(1, 0, 2)
    )
    grad_normed_one = lax.psum_scatter(
        contract_cols(grad_qkv_rows, qkv_joined).astype(jnp.bfloat16),
        "tensor",
        scatter_dimension=0,
        tiled=True,
    ).astype(jnp.float32)
    grad_token_norm, grad_gain_one, grad_shift_one = normalize_back(
        grad_normed_one, scaled_one, inverse_one, segment(0)
    )
    token_grad = (grad_mid + grad_token_norm).reshape(tokens.shape)
    rel_own = grad_tables.reshape(2, 64, head_size)[:, : rel_tables.shape[1]]
    width_zeros = jnp.zeros((model_width,), SINGLE)
    grad_small = jnp.concatenate(
        [
            grad_gain_one,
            grad_shift_one,
            lax.dynamic_update_slice_in_dim(
                width_zeros, grad_query_bias, tensor_index * head_width, 0
            ),
            lax.dynamic_update_slice_in_dim(
                width_zeros, grad_value_bias, tensor_index * head_width, 0
            ),
            grad_out_bias,
            grad_gain_two,
            grad_shift_two,
            grad_reduce_bias,
            expand_bias_full,
        ]
    )
    devices = lax.axis_size("dp") * tensor_count
    rel_flat = rel_own.reshape(-1)
    rel_piece = -(-rel_flat.shape[0] // devices)
    rel_flat = jnp.pad(rel_flat, (0, rel_piece * devices - rel_flat.shape[0]))
    packed = jnp.concatenate(
        [grad_small.reshape(devices, piece), rel_flat.reshape(devices, rel_piece)], axis=1
    )
    small_sum = lax.psum_scatter(
        jax.vmap(as_tiles)(packed), ("dp", "tensor"), scatter_dimension=0, tiled=False
    )
    gains_grad = small_sum.reshape(-1)[:piece]
    rel_grad = lax.all_gather(small_sum, ("dp", "tensor"), axis=0, tiled=False)
    rel_grad = rel_grad.reshape(devices, TILE)[:, piece : piece + rel_piece].reshape(-1)
    rel_grad = rel_grad[: rel_tables.size].reshape(rel_tables.shape)
    qkv_grad, out_grad, expand_grad, reduce_grad = (
        lax.psum_scatter(grad_qkv.astype(NARROW), "dp", scatter_dimension=1, tiled=True).astype(SINGLE),
        lax.psum_scatter(grad_out.astype(NARROW), "dp", scatter_dimension=1, tiled=True).astype(SINGLE),
        lax.psum_scatter(grad_expand.astype(NARROW), "dp", scatter_dimension=0, tiled=True).astype(SINGLE),
        lax.psum_scatter(grad_reduce.astype(NARROW), "dp", scatter_dimension=1, tiled=True).astype(SINGLE),
    )
    new_qkv, moment_qkv, average_qkv = advance(
        qkv_weight, qkv_moment, qkv_average, qkv_grad, RATE_MAIN
    )
    new_out, moment_out, average_out = advance(
        out_weight, out_moment, out_average, out_grad, RATE_MAIN
    )
    new_expand, moment_expand, average_expand = advance(
        expand_weight, expand_moment, expand_average, expand_grad, RATE_MAIN
    )
    new_reduce, moment_reduce, average_reduce = advance(
        reduce_weight, reduce_moment, reduce_average, reduce_grad, RATE_MAIN
    )
    new_gains, moment_gains, average_gains = advance(
        gains_biases, gains_moment, gains_average, gains_grad, RATE_MAIN
    )
    new_rel, moment_rel, average_rel = advance(
        rel_tables, rel_moment, rel_average, rel_grad, RATE_TABLES
    )
    return (
        block_out,
        token_grad,
        qkv_grad,
        out_grad,
        expand_grad,
        reduce_grad,
        gains_grad,
        rel_grad,
        new_qkv,
        new_out,
        new_expand,
        new_reduce,
        new_gains,
        new_rel,
        moment_qkv,
        moment_out,
        moment_expand,
        moment_reduce,
        moment_gains,
        moment_rel,
        average_qkv,
        average_out,
        average_expand,
        average_reduce,
        average_gains,
        average_rel,
    )


def solution(mesh):
    placed = (
        P("tensor", "dp", None),
        P("tensor", "dp", None),
        P(None, "dp", "tensor"),
        P("tensor", "dp"),
        P("dp", "tensor"),
        P("tensor", "dp"),
        P(("dp", "tensor")),
        P(),
        P(None, "dp", "tensor"),
        P("tensor", "dp"),
        P("dp", "tensor"),
        P("tensor", "dp"),
        P(("dp", "tensor")),
        P(),
        P(None, "dp", "tensor"),
        P("tensor", "dp"),
        P("dp", "tensor"),
        P("tensor", "dp"),
        P(("dp", "tensor")),
        P(),
    )
    return jax.shard_map(
        local,
        mesh=mesh,
        in_specs=placed,
        out_specs=(
            P("tensor", "dp", None),
            P("tensor", "dp", None),
            P(None, "dp", "tensor"),
            P("tensor", "dp"),
            P("dp", "tensor"),
            P("tensor", "dp"),
            P(("dp", "tensor")),
            P(),
            P(None, "dp", "tensor"),
            P("tensor", "dp"),
            P("dp", "tensor"),
            P("tensor", "dp"),
            P(("dp", "tensor")),
            P(),
            P(None, "dp", "tensor"),
            P("tensor", "dp"),
            P("dp", "tensor"),
            P("tensor", "dp"),
            P(("dp", "tensor")),
            P(),
            P(None, "dp", "tensor"),
            P("tensor", "dp"),
            P("dp", "tensor"),
            P("tensor", "dp"),
            P(("dp", "tensor")),
            P(),
        ),
        check_vma=False,
    )
```

```python
import functools
import jax
import jax.numpy as jnp
from jax import lax
from jax.experimental import pallas as pl
from jax.experimental.pallas import tpu as pltpu
from jax.sharding import PartitionSpec as P

EPSILON = 1e-06
MOMENTUM = 0.5
AVERAGING = 0.5
RATE_MAIN = 0.0003
RATE_TABLES = 0.01
NARROW = jnp.bfloat16
SINGLE = jnp.float32


def normalize(values, gain_row, shift_row):
    center = values - jnp.mean(values, axis=-1, keepdims=True)
    inverse = lax.rsqrt(jnp.mean(center * center, axis=-1, keepdims=True) + EPSILON)
    scaled = center * inverse
    return (scaled * gain_row + shift_row, scaled, inverse)


def normalize_back(grad_output, scaled, inverse, gain_row):
    grad_scaled = grad_output * gain_row
    mean_plain = jnp.mean(grad_scaled, axis=-1, keepdims=True)
    mean_cross = jnp.mean(grad_scaled * scaled, axis=-1, keepdims=True)
    grad_values = inverse * (grad_scaled - mean_plain - scaled * mean_cross)
    return (grad_values, jnp.sum(grad_output * scaled, axis=0), jnp.sum(grad_output, axis=0))


def gelu_slope(values):
    cumulative = 0.5 * (1.0 + lax.erf(values * 0.7071067811865476))
    density = 0.3989422804014327 * jnp.exp(-0.5 * values * values)
    return cumulative + values * density


def contract_rows(left_side, right_side):
    return lax.dot_general(
        left_side, right_side, (((0,), (0,)), ((), ())), preferred_element_type=SINGLE
    )


def contract_cols(left_side, right_side):
    return lax.dot_general(
        left_side, right_side, (((1,), (1,)), ((), ())), preferred_element_type=SINGLE
    )


def dot_nt(left, right):
    return lax.dot_general(left, right, (((1,), (1,)), ((), ())), preferred_element_type=SINGLE)


def dot_tn(left, right):
    return lax.dot_general(left, right, (((0,), (0,)), ((), ())), preferred_element_type=SINGLE)


def dot_nn(left, right):
    return lax.dot_general(left, right, (((1,), (0,)), ((), ())), preferred_element_type=SINGLE)


def forward_kernel(
    heads, size, grid_side, block, qkv_ref, table_ref, hot_ref,
    out_ref, bias_ref, lse_ref, query_ext, key_ext, bias_wide, context_t,
):
    seq = qkv_ref.shape[1]
    scale = size ** (-0.5)
    lane = lax.broadcasted_iota(jnp.int32, (grid_side, 128), 1)
    query_ext[:, 0:128] = jnp.zeros((seq, 128), NARROW)
    key_ext[:, 0:128] = jnp.zeros((seq, 128), NARROW)
    key_ext[:, 128:256] = hot_ref[...]
    for head in range(heads):
        low = head * size
        query = qkv_ref[0, :, low : low + size]
        value = qkv_ref[2, :, low : low + size]
        query_ext[:, 0:size] = query
        key_ext[:, 0:size] = qkv_ref[1, :, low : low + size]
        bias_wide[...] = dot_nt(query, table_ref[...])
        for row in range(grid_side):
            rows = pl.ds(row * grid_side, grid_side)
            group = bias_wide[rows, :]
            part_row = pltpu.roll(group, (128 - grid_side + 1 + row) % 128, 1)
            part_col = pltpu.roll(group, 65 - 32 + grid_side, 1, stride=1, stride_axis=0)
            both = jnp.where(
                lane < grid_side, part_row, jnp.where(lane < 2 * grid_side, part_col, 0.0)
            ) * (size ** 0.5)
            high = both.astype(NARROW).astype(SINGLE)
            rest = pltpu.roll(both - high, 64, 1)
            mixed = jnp.where(lane < 64, high, rest).astype(NARROW)
            query_ext[rows, 128:256] = mixed
        bias_ref[head] = query_ext[:, 128:256]
        for start in range(0, seq, block):
            scores = dot_nt(key_ext[...], query_ext[start : start + block, :])
            highest = jnp.max(scores, axis=0, keepdims=True)
            powers = jnp.exp((scores - highest) * scale)
            total = jnp.sum(powers, axis=0, keepdims=True)
            weights = (powers * (1.0 / total)).astype(NARROW)
            lse_ref[head, :, start : start + block] = highest * scale + jnp.log(total)
            context_t[low : low + size, start : start + block] = dot_tn(value, weights)
    out_ref[...] = context_t[...].T.astype(NARROW)


def backward_kernel(
    heads, size, grid_side, block, qkv_ref, grad_ref, bias_ref, lse_ref, table_ref, hot_ref, rev_ref,
    out_ref, rel_ref, query_ext, key_ext, key_rev, spread, grad_keys, grad_values, grad_query,
):
    seq = qkv_ref.shape[1]
    scale = size ** (-0.5)
    lane = lax.broadcasted_iota(jnp.int32, (grid_side, 128), 1)
    query_ext[:, 0:128] = jnp.zeros((seq, 128), NARROW)
    key_ext[:, 0:128] = jnp.zeros((seq, 128), NARROW)
    key_ext[:, 128:256] = hot_ref[...]
    key_rev[:, 0:128] = jnp.zeros((seq, 128), NARROW)
    key_rev[:, 128:256] = rev_ref[...]
    rel_total = jnp.zeros(rel_ref.shape, SINGLE)
    for head in range(heads):
        low = head * size
        query = qkv_ref[0, :, low : low + size]
        key = qkv_ref[1, :, low : low + size]
        value = qkv_ref[2, :, low : low + size]
        grad = grad_ref[:, low : low + size]
        query_ext[:, 0:size] = query
        query_ext[:, 128:256] = bias_ref[head]
        key_ext[:, 0:size] = key
        key_rev[:, 0:size] = key
        for start in range(0, seq, block):
            part = slice(start, start + block)
            scores = dot_nt(key_ext[...], query_ext[part, :])
            soft = jnp.exp(scores * scale - lse_ref[head, :, part])
            grad_part = grad[part]
            grad_soft = dot_nt(value, grad_part)
            inner = jnp.sum(soft * grad_soft, axis=0, keepdims=True)
            grad_scores = (soft * (grad_soft - inner)).astype(NARROW)
            add_values = dot_nn(soft.astype(NARROW), grad_part)
            add_keys = dot_nn(grad_scores, query[part])
            if start == 0:
                grad_values[...] = add_values
                grad_keys[...] = add_keys
            else:
                grad_values[...] += add_values
                grad_keys[...] += add_keys
            turned = dot_tn(key_rev[...], grad_scores).T
            grad_query[part, :] = turned[:, 0:128]
            sums = turned[:, 128:256].astype(NARROW).astype(SINGLE)
            for inside in range(block // grid_side):
                row = start // grid_side + inside
                group = sums[inside * grid_side : (inside + 1) * grid_side]
                part_row = jnp.where(lane < grid_side, group, 0.0)
                part_col = jnp.where((lane >= grid_side) & (lane < 2 * grid_side), group, 0.0)
                if row:
                    part_row = pltpu.roll(part_row, row, 1)
                part_col = pltpu.roll(part_col, 64 - grid_side, 1, stride=1, stride_axis=0)
                spread[row * grid_side : (row + 1) * grid_side, :] = (part_row + part_col).astype(NARROW)
        total_query = grad_query[:, 0:size] * scale + dot_nn(spread[...], table_ref[...])
        out_ref[0, :, low : low + size] = total_query.astype(NARROW)
        out_ref[1, :, low : low + size] = (grad_keys[...] * scale).astype(NARROW)
        out_ref[2, :, low : low + size] = grad_values[...].astype(NARROW)
        rel_total = rel_total + dot_tn(spread[...], query)
    rel_ref[...] = rel_total


def attention_tables(rel_low, grid_side):
    offsets = rel_low.shape[1]
    pad = ((0, 0), (0, 64 - offsets), (0, 0))
    plain = jnp.pad(rel_low, pad).reshape(128, -1)
    turned = jnp.pad(rel_low[:, ::-1], pad).reshape(128, -1)
    seq = grid_side * grid_side
    token = lax.broadcasted_iota(jnp.int32, (seq, 128), 0)
    lane = lax.broadcasted_iota(jnp.int32, (seq, 128), 1)
    inside = lane % 64
    row, col = (token // grid_side, token % grid_side)
    hot = jnp.where(inside < grid_side, inside == row, inside - grid_side == col)
    hot = (hot & (inside < 2 * grid_side)).astype(NARROW)
    back = jnp.where(lane < grid_side, grid_side - 1 - lane == row, 2 * grid_side - 1 - lane == col)
    back = (back & (lane < 2 * grid_side)).astype(NARROW)
    return plain, turned, hot, back


def whole_vmem(count):
    return [pl.BlockSpec(memory_space=pltpu.VMEM)] * count


def attend_forward(qkv_rows, turned, hot, heads, size, grid_side):
    seq = qkv_rows.shape[1]
    block = min(256, seq)
    return pl.pallas_call(
        functools.partial(forward_kernel, heads, size, grid_side, block),
        out_shape=(
            jax.ShapeDtypeStruct((seq, heads * size), NARROW),
            jax.ShapeDtypeStruct((heads, seq, 128), NARROW),
            jax.ShapeDtypeStruct((heads, 1, seq), SINGLE),
        ),
        in_specs=whole_vmem(3),
        out_specs=tuple(whole_vmem(3)),
        scratch_shapes=[
            pltpu.VMEM((seq, 256), NARROW),
            pltpu.VMEM((seq, 256), NARROW),
            pltpu.VMEM((seq, 128), SINGLE),
            pltpu.VMEM((heads * size, seq), SINGLE),
        ],
        compiler_params=pltpu.CompilerParams(vmem_limit_bytes=40 << 20),
        name="attend_forward",
    )(qkv_rows, turned, hot)


def attend_backward(qkv_rows, grad_rows, bias, lse, plain, hot, back, heads, size, grid_side):
    seq = qkv_rows.shape[1]
    block = min(256, seq)
    return pl.pallas_call(
        functools.partial(backward_kernel, heads, size, grid_side, block),
        out_shape=(
            jax.ShapeDtypeStruct((3, seq, heads * size), NARROW),
            jax.ShapeDtypeStruct((128, size), SINGLE),
        ),
        in_specs=whole_vmem(7),
        out_specs=tuple(whole_vmem(2)),
        scratch_shapes=[
            pltpu.VMEM((seq, 256), NARROW),
            pltpu.VMEM((seq, 256), NARROW),
            pltpu.VMEM((seq, 256), NARROW),
            pltpu.VMEM((seq, 128), NARROW),
            pltpu.VMEM((seq, size), SINGLE),
            pltpu.VMEM((seq, size), SINGLE),
            pltpu.VMEM((seq, 128), SINGLE),
        ],
        compiler_params=pltpu.CompilerParams(vmem_limit_bytes=48 << 20),
        name="attend_backward",
    )(qkv_rows, grad_rows, bias, lse, plain, hot, back)


MESH_IDS = pl.DeviceIdType.MESH


def place_of(index, inner):
    return (index // inner, index % inner)


def greet_all(me, count, inner):
    barrier = pltpu.get_barrier_semaphore()

    def signal(step, carry):
        pl.semaphore_signal(
            barrier, inc=1, device_id=place_of((me + step) % count, inner), device_id_type=MESH_IDS
        )
        return carry

    lax.fori_loop(1, count, signal, 0)
    pl.semaphore_wait(barrier, count - 1)


def exchange(me, count, inner, source, target, send_sem, recv_sem):
    def piece(step):
        other = (me + step) % count
        return pltpu.make_async_remote_copy(
            src_ref=source(other),
            dst_ref=target.at[me],
            send_sem=send_sem.at[step],
            recv_sem=recv_sem.at[step],
            device_id=place_of(other, inner),
            device_id_type=MESH_IDS,
        )

    def start(step, carry):
        piece(step).start()
        return carry

    def finish(step, carry):
        sender = (me + count - step) % count
        pltpu.make_async_remote_copy(
            src_ref=source(sender),
            dst_ref=target.at[sender],
            send_sem=send_sem.at[step],
            recv_sem=recv_sem.at[step],
            device_id=place_of(sender, inner),
            device_id_type=MESH_IDS,
        ).wait_recv()
        piece(step).wait_send()
        return carry

    lax.fori_loop(1, count, start, 0)
    lax.fori_loop(1, count, finish, 0)


def small_gather_kernel(outer, inner, own_ref, all_ref, send_sem, recv_sem):
    count = outer * inner
    me = lax.axis_index("dp") * inner + lax.axis_index("tensor")
    greet_all(me, count, inner)
    all_ref[me] = own_ref[...]
    exchange(me, count, inner, lambda other: own_ref, all_ref, send_sem, recv_sem)


def small_sum_kernel(
    outer, inner, packed_ref, total_ref, all_ref, landing, send_one, recv_one, send_two, recv_two
):
    count = outer * inner
    me = lax.axis_index("dp") * inner + lax.axis_index("tensor")
    greet_all(me, count, inner)
    landing[me] = packed_ref[me]
    exchange(me, count, inner, lambda other: packed_ref.at[other], landing, send_one, recv_one)
    total = jnp.sum(landing[...], axis=0)
    total_ref[...] = total
    all_ref[me] = total
    exchange(me, count, inner, lambda other: total_ref, all_ref, send_two, recv_two)


def small_gather(own, outer, inner, collective_id):
    count = outer * inner
    return pl.pallas_call(
        functools.partial(small_gather_kernel, outer, inner),
        out_shape=jax.ShapeDtypeStruct((count,) + own.shape, own.dtype),
        in_specs=whole_vmem(1),
        out_specs=whole_vmem(1)[0],
        scratch_shapes=[pltpu.SemaphoreType.DMA((count,))] * 2,
        compiler_params=pltpu.CompilerParams(collective_id=collective_id, has_side_effects=True),
        name="small_gather",
    )(own)


def small_sum(packed, outer, inner, collective_id):
    count = outer * inner
    return pl.pallas_call(
        functools.partial(small_sum_kernel, outer, inner),
        out_shape=(
            jax.ShapeDtypeStruct(packed.shape[1:], packed.dtype),
            jax.ShapeDtypeStruct(packed.shape, packed.dtype),
        ),
        in_specs=whole_vmem(1),
        out_specs=tuple(whole_vmem(2)),
        scratch_shapes=[pltpu.VMEM(packed.shape, packed.dtype)]
        + [pltpu.SemaphoreType.DMA((count,))] * 4,
        compiler_params=pltpu.CompilerParams(collective_id=collective_id, has_side_effects=True),
        name="small_sum",
    )(packed)


def greet_line(me, parts):
    barrier = pltpu.get_barrier_semaphore()

    @pl.when(me > 0)
    def _():
        pl.semaphore_signal(barrier, inc=1, device_id={"tensor": me - 1}, device_id_type=MESH_IDS)

    @pl.when(me < parts - 1)
    def _():
        pl.semaphore_signal(barrier, inc=1, device_id={"tensor": me + 1}, device_id_type=MESH_IDS)

    @pl.when((me > 0) & (me < parts - 1))
    def _():
        pl.semaphore_wait(barrier, 2)

    @pl.when((me == 0) | (me == parts - 1))
    def _():
        pl.semaphore_wait(barrier, 1)


def gather_kernel(parts, chunks, inputs, finish_rows, own_ref, *refs):
    extra = refs[:inputs]
    all_ref = refs[inputs]
    results = refs[inputs + 1 : -2]
    send_sem, recv_sem = refs[-2:]
    me = lax.axis_index("tensor")
    rows = own_ref.shape[0]
    chunk = rows // chunks
    greet_line(me, parts)

    def block(shard, piece):
        return all_ref.at[pl.ds(pl.multiple_of(shard * rows + piece * chunk, chunk), chunk)]

    def outgoing(way, step, piece):
        shard = me - step if way == 0 else me + step
        source = own_ref.at[pl.ds(piece * chunk, chunk)] if step == 0 else block(shard, piece)
        return pltpu.make_async_remote_copy(
            src_ref=source,
            dst_ref=block(shard, piece),
            send_sem=send_sem.at[way, step, piece],
            recv_sem=recv_sem.at[way, step + 1, piece],
            device_id={"tensor": me + 1 if way == 0 else me - 1},
            device_id_type=MESH_IDS,
        )

    def incoming(way, step, piece):
        shard = me - step if way == 0 else me + step
        return pltpu.make_async_remote_copy(
            src_ref=block(shard, piece),
            dst_ref=block(shard, piece),
            send_sem=send_sem.at[way, step, piece],
            recv_sem=recv_sem.at[way, step, piece],
            device_id={"tensor": me - 1 if way == 0 else me + 1},
            device_id_type=MESH_IDS,
        )

    def held(way, step):
        return me - step >= 0 if way == 0 else me + step < parts

    def passes(way, step):
        return held(way, step) & ((me < parts - 1) if way == 0 else (me > 0))

    for step in range(parts):
        for piece in range(chunks):
            for way in range(2):
                if step:

                    @pl.when(held(way, step))
                    def _():
                        incoming(way, step, piece).wait_recv()

                if step < parts - 1:

                    @pl.when(passes(way, step))
                    def _():
                        outgoing(way, step, piece).start()

        if step == 0:
            mine = pl.ds(pl.multiple_of(me * rows, rows), rows)
            all_ref[mine, :] = own_ref[...]
            finish_rows(own_ref[...], mine, extra, results)
        else:
            for way in range(2):

                @pl.when(held(way, step))
                def _():
                    shard = me - step if way == 0 else me + step
                    place = pl.ds(pl.multiple_of(shard * rows, rows), rows)
                    finish_rows(all_ref[place, :], place, extra, results)

    for step in range(parts - 1):
        for piece in range(chunks):
            for way in range(2):

                @pl.when(passes(way, step))
                def _():
                    outgoing(way, step, piece).wait_send()


def gather_rows(own, extra, results, finish_rows, parts, collective_id, name):
    chunks = 4
    return pl.pallas_call(
        functools.partial(gather_kernel, parts, chunks, len(extra), finish_rows),
        out_shape=(jax.ShapeDtypeStruct((parts * own.shape[0], own.shape[1]), own.dtype),)
        + tuple(results),
        in_specs=whole_vmem(1 + len(extra)),
        out_specs=tuple(whole_vmem(1 + len(results))),
        scratch_shapes=[
            pltpu.SemaphoreType.DMA((2, parts, chunks)),
            pltpu.SemaphoreType.DMA((2, parts, chunks)),
        ],
        compiler_params=pltpu.CompilerParams(
            collective_id=collective_id, has_side_effects=True, vmem_limit_bytes=40 << 20
        ),
        name=name,
    )(own, *extra)


def scatter_kernel(
    parts, chunks, turned, left_ref, weight_ref, out_ref, product, landing, send_sem, recv_sem
):
    me = lax.axis_index("tensor")
    rows = out_ref.shape[0]
    chunk = rows // chunks
    greet_line(me, parts)

    def own_block(shard, piece):
        return pl.ds(pl.multiple_of(shard * rows + piece * chunk, chunk), chunk)

    def outgoing(way, far, piece, source):
        return pltpu.make_async_remote_copy(
            src_ref=source,
            dst_ref=landing.at[way, far - 1, pl.ds(piece * chunk, chunk)],
            send_sem=send_sem.at[way, far, piece],
            recv_sem=recv_sem.at[way, far - 1, piece],
            device_id={"tensor": me + 1 if way == 0 else me - 1},
            device_id_type=MESH_IDS,
        )

    def wait_landing(way, far, piece):
        spot = landing.at[way, far, pl.ds(piece * chunk, chunk)]
        pltpu.make_async_remote_copy(
            src_ref=spot,
            dst_ref=spot,
            send_sem=send_sem.at[way, far, piece],
            recv_sem=recv_sem.at[way, far, piece],
            device_id={"tensor": me - 1 if way == 0 else me + 1},
            device_id_type=MESH_IDS,
        ).wait_recv()

    def first(way):
        return me == 0 if way == 0 else me == parts - 1

    for step in range(parts):
        shard = jnp.where(me < parts // 2, parts - 1 - step, step)
        place = pl.ds(pl.multiple_of(shard * rows, rows), rows)
        total = None
        for part in range(left_ref.shape[0]):
            term = (dot_nt if turned else dot_nn)(left_ref[part, place, :], weight_ref[part])
            total = term if total is None else total + term
        product[place, :] = total.astype(NARROW)
        far = parts - 1 - step
        if far:
            for way in range(2):

                @pl.when(first(way))
                def _():
                    shard = me + far if way == 0 else me - far
                    for piece in range(chunks):
                        outgoing(way, far, piece, product.at[own_block(shard, piece)]).start()

    def relays(way, far):
        return (~first(way)) & ((me + far < parts) if way == 0 else (me - far >= 0))

    for far in range(parts - 2, 0, -1):
        for piece in range(chunks):
            for way in range(2):

                @pl.when(relays(way, far))
                def _():
                    wait_landing(way, far, piece)
                    shard = me + far if way == 0 else me - far
                    spot = (way, far, pl.ds(piece * chunk, chunk))
                    landing[spot] = (
                        landing[spot].astype(SINGLE)
                        + product[own_block(shard, piece), :].astype(SINGLE)
                    ).astype(NARROW)
                    outgoing(way, far, piece, landing.at[spot]).start()

    for piece in range(chunks):
        place = pl.ds(piece * chunk, chunk)
        out_ref[place, :] = product[own_block(me, piece), :].astype(SINGLE)
        for way in range(2):

            @pl.when(~first(way))
            def _():
                wait_landing(way, 0, piece)
                out_ref[place, :] += landing[way, 0, place].astype(SINGLE)

    for far in range(parts - 1, 0, -1):
        for piece in range(chunks):
            for way in range(2):
                shard = me + far if way == 0 else me - far

                @pl.when(first(way))
                def _():
                    outgoing(way, far, piece, product.at[own_block(shard, piece)]).wait_send()

                if far < parts - 1:

                    @pl.when(relays(way, far))
                    def _():
                        spot = landing.at[way, far, pl.ds(piece * chunk, chunk)]
                        outgoing(way, far, piece, spot).wait_send()


def scatter_rows(left, weight, turned, parts, collective_id, name):
    chunks = 4
    total_rows = left.shape[1]
    rows = total_rows // parts
    width = weight.shape[1] if turned else weight.shape[2]
    return pl.pallas_call(
        functools.partial(scatter_kernel, parts, chunks, turned),
        out_shape=jax.ShapeDtypeStruct((rows, width), SINGLE),
        in_specs=whole_vmem(2),
        out_specs=whole_vmem(1)[0],
        scratch_shapes=[
            pltpu.VMEM((total_rows, width), NARROW),
            pltpu.VMEM((2, parts - 1, rows, width), NARROW),
            pltpu.SemaphoreType.DMA((2, parts, chunks)),
            pltpu.SemaphoreType.DMA((2, parts, chunks)),
        ],
        compiler_params=pltpu.CompilerParams(
            collective_id=collective_id, has_side_effects=True, vmem_limit_bytes=40 << 20
        ),
        name=name,
    )(left, weight)


def project_rows(values, place, extra, results):
    weight_ref, bias_ref = extra
    for part in range(weight_ref.shape[0]):
        total = dot_nn(values, weight_ref[part]) + bias_ref[part]
        results[0][part, place, :] = total.astype(NARROW)


def expand_rows(values, place, extra, results):
    weight_ref, bias_ref = extra
    hidden = dot_nn(values, weight_ref[...]) + bias_ref[...]
    cumulative = 0.5 * (1.0 + lax.erf(hidden * 0.7071067811865476))
    density = 0.3989422804014327 * jnp.exp(-0.5 * hidden * hidden)
    results[0][place, :] = (hidden * cumulative).astype(NARROW)
    results[1][place, :] = cumulative + hidden * density


def context_grad_rows(values, place, extra, results):
    results[0][place, :] = dot_nt(values, extra[0][...]).astype(NARROW)


TILE = 1024


def as_tiles(vector):
    return jnp.pad(vector, (0, TILE - vector.shape[0])).reshape(8, 128)


def advance(weight, moment, average, gradient, rate_value):
    new_moment = MOMENTUM * moment + gradient
    new_weight = weight - rate_value * (gradient + MOMENTUM * new_moment)
    new_average = AVERAGING * average + (1.0 - AVERAGING) * new_weight
    return (new_weight, new_moment, new_average)


def local(
    tokens,
    cotangent,
    qkv_weight,
    out_weight,
    expand_weight,
    reduce_weight,
    gains_biases,
    rel_tables,
    qkv_moment,
    out_moment,
    expand_moment,
    reduce_moment,
    gains_moment,
    rel_moment,
    qkv_average,
    out_average,
    expand_average,
    reduce_average,
    gains_average,
    rel_average,
):
    local_seq, local_images, model_width = tokens.shape
    tensor_count = lax.axis_size("tensor")
    tensor_index = lax.axis_index("tensor")
    local_rows = local_seq * local_images
    seq_length = local_seq * tensor_count
    head_width = qkv_weight.shape[2]
    hidden_width = expand_weight.shape[1]
    head_size = rel_tables.shape[2]
    grid_side = (rel_tables.shape[1] + 1) // 2
    qkv_full, out_full, expand_full, reduce_full = (
        lax.all_gather(qkv_weight.astype(NARROW), "dp", axis=1, tiled=True),
        lax.all_gather(out_weight.astype(NARROW), "dp", axis=1, tiled=True),
        lax.all_gather(expand_weight.astype(NARROW), "dp", axis=0, tiled=True),
        lax.all_gather(reduce_weight.astype(NARROW), "dp", axis=1, tiled=True),
    )
    piece = gains_biases.shape[0]
    outer = lax.axis_size("dp")
    params_all = small_gather(as_tiles(gains_biases), outer, tensor_count, 0)
    params_all = params_all.reshape(-1, TILE)[:, :piece].reshape(-1)

    def segment(position):
        return params_all[position * model_width : (position + 1) * model_width]

    query_bias = lax.dynamic_slice_in_dim(
        params_all, 2 * model_width + tensor_index * head_width, head_width
    )
    value_bias = lax.dynamic_slice_in_dim(
        params_all, 3 * model_width + tensor_index * head_width, head_width
    )
    heads = head_width // head_size
    plain, turned, hot, back = attention_tables(rel_tables.astype(NARROW), grid_side)
    token_rows = tokens.reshape(local_rows, model_width).astype(SINGLE)
    normed_one, scaled_one, inverse_one = normalize(token_rows, segment(0), segment(1))
    qkv_bias = jnp.stack([query_bias, jnp.zeros((head_width,), SINGLE), value_bias])
    gathered_one, qkv_rows = gather_rows(
        normed_one.astype(NARROW),
        (qkv_full, qkv_bias[:, None]),
        (jax.ShapeDtypeStruct((3, seq_length, head_width), NARROW),),
        project_rows, tensor_count, 2, "gather_project",
    )
    context_rows, bias_wide, logsums = attend_forward(
        qkv_rows, turned, hot, heads, head_size, grid_side
    )
    attn_sum = scatter_rows(context_rows[None], out_full[None], False, tensor_count, 3, "scatter_out")
    mid_rows = token_rows + (attn_sum + segment(4))
    normed_two, scaled_two, inverse_two = normalize(mid_rows, segment(5), segment(6))
    normed_two_low = normed_two.astype(NARROW)
    expand_bias = lax.dynamic_slice_in_dim(
        params_all, 8 * model_width + tensor_index * hidden_width, hidden_width
    )
    gathered_two, hidden_low, hidden_slope = gather_rows(
        normed_two_low,
        (expand_full, expand_bias[None]),
        (
            jax.ShapeDtypeStruct((seq_length, hidden_width), NARROW),
            jax.ShapeDtypeStruct((seq_length, hidden_width), SINGLE),
        ),
        expand_rows, tensor_count, 4, "gather_expand",
    )
    mlp_sum = lax.psum_scatter(
        jnp.dot(hidden_low, reduce_full, preferred_element_type=SINGLE).astype(jnp.bfloat16),
        "tensor",
        scatter_dimension=0,
        tiled=True,
    ).astype(jnp.float32)
    block_rows = mid_rows + (mlp_sum + segment(7))
    block_out = block_rows.astype(NARROW).reshape(tokens.shape)
    cotangent_rows = cotangent.reshape(local_rows, model_width)
    grad_block = cotangent_rows.astype(SINGLE)
    grad_reduce_bias = jnp.sum(grad_block, axis=0)
    shard_rows = lax.all_gather(cotangent_rows, "tensor", axis=0, tiled=True)
    part_hidden = contract_cols(shard_rows, reduce_full)
    grad_hidden = part_hidden
    grad_hidden, grad_reduce = (grad_hidden, contract_rows(hidden_low, shard_rows))
    grad_pre = (grad_hidden * hidden_slope).astype(NARROW)
    grad_expand = contract_rows(gathered_two, grad_pre)
    grad_expand_bias = jnp.sum(grad_pre, axis=0, dtype=SINGLE)
    expand_bias_full = lax.dynamic_update_slice_in_dim(
        jnp.zeros((hidden_width * tensor_count,), SINGLE),
        grad_expand_bias,
        tensor_index * hidden_width,
        0,
    )
    grad_normed_two = scatter_rows(
        grad_pre[None], expand_full[None], True, tensor_count, 5, "scatter_expand"
    )
    grad_mid_norm, grad_gain_two, grad_shift_two = normalize_back(
        grad_normed_two, scaled_two, inverse_two, segment(5)
    )
    grad_mid = grad_block + grad_mid_norm
    grad_attn_low = grad_mid.astype(NARROW)
    grad_out_bias = jnp.sum(grad_attn_low, axis=0, dtype=SINGLE)
    shard_rows, grad_context = gather_rows(
        grad_attn_low,
        (out_full,),
        (jax.ShapeDtypeStruct((seq_length, head_width), NARROW),),
        context_grad_rows, tensor_count, 6, "gather_context",
    )
    grad_out = contract_rows(context_rows, shard_rows)
    grad_qkv_rows, grad_tables = attend_backward(
        qkv_rows, grad_context, bias_wide, logsums, plain, hot, back,
        heads, head_size, grid_side,
    )
    grad_query_bias = jnp.sum(grad_qkv_rows[0], axis=0, dtype=SINGLE)
    grad_value_bias = jnp.sum(grad_qkv_rows[2], axis=0, dtype=SINGLE)
    grad_qkv = jnp.stack([contract_rows(gathered_one, grad_qkv_rows[part]) for part in range(3)])
    grad_normed_one = scatter_rows(
        grad_qkv_rows, qkv_full, True, tensor_count, 7, "scatter_qkv"
    )
    grad_token_norm, grad_gain_one, grad_shift_one = normalize_back(
        grad_normed_one, scaled_one, inverse_one, segment(0)
    )
    token_grad = (grad_mid + grad_token_norm).reshape(tokens.shape)
    rel_own = grad_tables.reshape(2, 64, head_size)[:, : rel_tables.shape[1]]
    width_zeros = jnp.zeros((model_width,), SINGLE)
    grad_small = jnp.concatenate(
        [
            grad_gain_one,
            grad_shift_one,
            lax.dynamic_update_slice_in_dim(
                width_zeros, grad_query_bias, tensor_index * head_width, 0
            ),
            lax.dynamic_update_slice_in_dim(
                width_zeros, grad_value_bias, tensor_index * head_width, 0
            ),
            grad_out_bias,
            grad_gain_two,
            grad_shift_two,
            grad_reduce_bias,
            expand_bias_full,
        ]
    )
    devices = lax.axis_size("dp") * tensor_count
    rel_flat = rel_own.reshape(-1)
    rel_piece = -(-rel_flat.shape[0] // devices)
    rel_flat = jnp.pad(rel_flat, (0, rel_piece * devices - rel_flat.shape[0]))
    packed = jnp.concatenate(
        [grad_small.reshape(devices, piece), rel_flat.reshape(devices, rel_piece)], axis=1
    )
    own_sum, rel_grad = small_sum(jax.vmap(as_tiles)(packed), outer, tensor_count, 1)
    gains_grad = own_sum.reshape(-1)[:piece]
    rel_grad = rel_grad.reshape(devices, TILE)[:, piece : piece + rel_piece].reshape(-1)
    rel_grad = rel_grad[: rel_tables.size].reshape(rel_tables.shape)
    qkv_grad, out_grad, expand_grad, reduce_grad = (
        lax.psum_scatter(grad_qkv.astype(NARROW), "dp", scatter_dimension=1, tiled=True).astype(SINGLE),
        lax.psum_scatter(grad_out.astype(NARROW), "dp", scatter_dimension=1, tiled=True).astype(SINGLE),
        lax.psum_scatter(grad_expand.astype(NARROW), "dp", scatter_dimension=0, tiled=True).astype(SINGLE),
        lax.psum_scatter(grad_reduce.astype(NARROW), "dp", scatter_dimension=1, tiled=True).astype(SINGLE),
    )
    new_qkv, moment_qkv, average_qkv = advance(
        qkv_weight, qkv_moment, qkv_average, qkv_grad, RATE_MAIN
    )
    new_out, moment_out, average_out = advance(
        out_weight, out_moment, out_average, out_grad, RATE_MAIN
    )
    new_expand, moment_expand, average_expand = advance(
        expand_weight, expand_moment, expand_average, expand_grad, RATE_MAIN
    )
    new_reduce, moment_reduce, average_reduce = advance(
        reduce_weight, reduce_moment, reduce_average, reduce_grad, RATE_MAIN
    )
    new_gains, moment_gains, average_gains = advance(
        gains_biases, gains_moment, gains_average, gains_grad, RATE_MAIN
    )
    new_rel, moment_rel, average_rel = advance(
        rel_tables, rel_moment, rel_average, rel_grad, RATE_TABLES
    )
    return (
        block_out,
        token_grad,
        qkv_grad,
        out_grad,
        expand_grad,
        reduce_grad,
        gains_grad,
        rel_grad,
        new_qkv,
        new_out,
        new_expand,
        new_reduce,
        new_gains,
        new_rel,
        moment_qkv,
        moment_out,
        moment_expand,
        moment_reduce,
        moment_gains,
        moment_rel,
        average_qkv,
        average_out,
        average_expand,
        average_reduce,
        average_gains,
        average_rel,
    )


def solution(mesh):
    placed = (
        P("tensor", "dp", None),
        P("tensor", "dp", None),
        P(None, "dp", "tensor"),
        P("tensor", "dp"),
        P("dp", "tensor"),
        P("tensor", "dp"),
        P(("dp", "tensor")),
        P(),
        P(None, "dp", "tensor"),
        P("tensor", "dp"),
        P("dp", "tensor"),
        P("tensor", "dp"),
        P(("dp", "tensor")),
        P(),
        P(None, "dp", "tensor"),
        P("tensor", "dp"),
        P("dp", "tensor"),
        P("tensor", "dp"),
        P(("dp", "tensor")),
        P(),
    )
    return jax.shard_map(
        local,
        mesh=mesh,
        in_specs=placed,
        out_specs=(
            P("tensor", "dp", None),
            P("tensor", "dp", None),
            P(None, "dp", "tensor"),
            P("tensor", "dp"),
            P("dp", "tensor"),
            P("tensor", "dp"),
            P(("dp", "tensor")),
            P(),
            P(None, "dp", "tensor"),
            P("tensor", "dp"),
            P("dp", "tensor"),
            P("tensor", "dp"),
            P(("dp", "tensor")),
            P(),
            P(None, "dp", "tensor"),
            P("tensor", "dp"),
            P("dp", "tensor"),
            P("tensor", "dp"),
            P(("dp", "tensor")),
            P(),
            P(None, "dp", "tensor"),
            P("tensor", "dp"),
            P("dp", "tensor"),
            P("tensor", "dp"),
            P(("dp", "tensor")),
            P(),
        ),
        check_vma=False,
    )
```

```python
import functools
import jax
import jax.numpy as jnp
from jax import lax
from jax.experimental import pallas as pl
from jax.experimental.pallas import tpu as pltpu
from jax.sharding import PartitionSpec as P

EPSILON = 1e-06
MOMENTUM = 0.5
AVERAGING = 0.5
RATE_MAIN = 0.0003
RATE_TABLES = 0.01
NARROW = jnp.bfloat16
SINGLE = jnp.float32


def normalize(values, gain_row, shift_row):
    center = values - jnp.mean(values, axis=-1, keepdims=True)
    inverse = lax.rsqrt(jnp.mean(center * center, axis=-1, keepdims=True) + EPSILON)
    scaled = center * inverse
    return (scaled * gain_row + shift_row, scaled, inverse)


def normalize_back(grad_output, scaled, inverse, gain_row):
    grad_scaled = grad_output * gain_row
    mean_plain = jnp.mean(grad_scaled, axis=-1, keepdims=True)
    mean_cross = jnp.mean(grad_scaled * scaled, axis=-1, keepdims=True)
    grad_values = inverse * (grad_scaled - mean_plain - scaled * mean_cross)
    return (grad_values, jnp.sum(grad_output * scaled, axis=0), jnp.sum(grad_output, axis=0))


def gelu_slope(values):
    cumulative = 0.5 * (1.0 + lax.erf(values * 0.7071067811865476))
    density = 0.3989422804014327 * jnp.exp(-0.5 * values * values)
    return cumulative + values * density


def contract_rows(left_side, right_side):
    return lax.dot_general(
        left_side, right_side, (((0,), (0,)), ((), ())), preferred_element_type=SINGLE
    )


def contract_cols(left_side, right_side):
    return lax.dot_general(
        left_side, right_side, (((1,), (1,)), ((), ())), preferred_element_type=SINGLE
    )


def dot_nt(left, right):
    return lax.dot_general(left, right, (((1,), (1,)), ((), ())), preferred_element_type=SINGLE)


def dot_tn(left, right):
    return lax.dot_general(left, right, (((0,), (0,)), ((), ())), preferred_element_type=SINGLE)


def dot_nn(left, right):
    return lax.dot_general(left, right, (((1,), (0,)), ((), ())), preferred_element_type=SINGLE)


def forward_kernel(
    heads, size, grid_side, block, qkv_ref, table_ref, hot_ref,
    out_ref, bias_ref, lse_ref, query_ext, key_ext, bias_wide, context_t,
):
    seq = qkv_ref.shape[1]
    scale = size ** (-0.5)
    lane = lax.broadcasted_iota(jnp.int32, (grid_side, 128), 1)
    query_ext[:, 0:128] = jnp.zeros((seq, 128), NARROW)
    key_ext[:, 0:128] = jnp.zeros((seq, 128), NARROW)
    key_ext[:, 128:256] = hot_ref[...]
    for head in range(heads):
        low = head * size
        query = qkv_ref[0, :, low : low + size]
        value = qkv_ref[2, :, low : low + size]
        query_ext[:, 0:size] = query
        key_ext[:, 0:size] = qkv_ref[1, :, low : low + size]
        bias_wide[...] = dot_nt(query, table_ref[...])
        for row in range(grid_side):
            rows = pl.ds(row * grid_side, grid_side)
            group = bias_wide[rows, :]
            part_row = pltpu.roll(group, (128 - grid_side + 1 + row) % 128, 1)
            part_col = pltpu.roll(group, 65 - 32 + grid_side, 1, stride=1, stride_axis=0)
            both = jnp.where(
                lane < grid_side, part_row, jnp.where(lane < 2 * grid_side, part_col, 0.0)
            ) * (size ** 0.5)
            high = both.astype(NARROW).astype(SINGLE)
            rest = pltpu.roll(both - high, 64, 1)
            mixed = jnp.where(lane < 64, high, rest).astype(NARROW)
            query_ext[rows, 128:256] = mixed
        bias_ref[head] = query_ext[:, 128:256]
        for start in range(0, seq, block):
            scores = dot_nt(key_ext[...], query_ext[start : start + block, :])
            highest = jnp.max(scores, axis=0, keepdims=True)
            powers = jnp.exp((scores - highest) * scale)
            total = jnp.sum(powers, axis=0, keepdims=True)
            weights = (powers * (1.0 / total)).astype(NARROW)
            lse_ref[head, :, start : start + block] = highest * scale + jnp.log(total)
            context_t[low : low + size, start : start + block] = dot_tn(value, weights)
    out_ref[...] = context_t[...].T.astype(NARROW)


def backward_kernel(
    heads, size, grid_side, block, qkv_ref, grad_ref, bias_ref, lse_ref, table_ref, hot_ref, rev_ref,
    out_ref, rel_ref, query_ext, key_ext, key_rev, spread, grad_keys, grad_values, grad_query,
):
    seq = qkv_ref.shape[1]
    scale = size ** (-0.5)
    lane = lax.broadcasted_iota(jnp.int32, (grid_side, 128), 1)
    query_ext[:, 0:128] = jnp.zeros((seq, 128), NARROW)
    key_ext[:, 0:128] = jnp.zeros((seq, 128), NARROW)
    key_ext[:, 128:256] = hot_ref[...]
    key_rev[:, 0:128] = jnp.zeros((seq, 128), NARROW)
    key_rev[:, 128:256] = rev_ref[...]
    rel_total = jnp.zeros(rel_ref.shape, SINGLE)
    for head in range(heads):
        low = head * size
        query = qkv_ref[0, :, low : low + size]
        key = qkv_ref[1, :, low : low + size]
        value = qkv_ref[2, :, low : low + size]
        grad = grad_ref[:, low : low + size]
        query_ext[:, 0:size] = query
        query_ext[:, 128:256] = bias_ref[head]
        key_ext[:, 0:size] = key
        key_rev[:, 0:size] = key
        for start in range(0, seq, block):
            part = slice(start, start + block)
            scores = dot_nt(key_ext[...], query_ext[part, :])
            soft = jnp.exp(scores * scale - lse_ref[head, :, part])
            grad_part = grad[part]
            grad_soft = dot_nt(value, grad_part)
            inner = jnp.sum(soft * grad_soft, axis=0, keepdims=True)
            grad_scores = (soft * (grad_soft - inner)).astype(NARROW)
            add_values = dot_nn(soft.astype(NARROW), grad_part)
            add_keys = dot_nn(grad_scores, query[part])
            if start == 0:
                grad_values[...] = add_values
                grad_keys[...] = add_keys
            else:
                grad_values[...] += add_values
                grad_keys[...] += add_keys
            turned = dot_tn(key_rev[...], grad_scores).T
            grad_query[part, :] = turned[:, 0:128]
            sums = turned[:, 128:256].astype(NARROW).astype(SINGLE)
            for inside in range(block // grid_side):
                row = start // grid_side + inside
                group = sums[inside * grid_side : (inside + 1) * grid_side]
                part_row = jnp.where(lane < grid_side, group, 0.0)
                part_col = jnp.where((lane >= grid_side) & (lane < 2 * grid_side), group, 0.0)
                if row:
                    part_row = pltpu.roll(part_row, row, 1)
                part_col = pltpu.roll(part_col, 64 - grid_side, 1, stride=1, stride_axis=0)
                spread[row * grid_side : (row + 1) * grid_side, :] = (part_row + part_col).astype(NARROW)
        total_query = grad_query[:, 0:size] * scale + dot_nn(spread[...], table_ref[...])
        out_ref[0, :, low : low + size] = total_query.astype(NARROW)
        out_ref[1, :, low : low + size] = (grad_keys[...] * scale).astype(NARROW)
        out_ref[2, :, low : low + size] = grad_values[...].astype(NARROW)
        rel_total = rel_total + dot_tn(spread[...], query)
    rel_ref[...] = rel_total


def attention_tables(rel_low, grid_side):
    offsets = rel_low.shape[1]
    pad = ((0, 0), (0, 64 - offsets), (0, 0))
    plain = jnp.pad(rel_low, pad).reshape(128, -1)
    turned = jnp.pad(rel_low[:, ::-1], pad).reshape(128, -1)
    seq = grid_side * grid_side
    token = lax.broadcasted_iota(jnp.int32, (seq, 128), 0)
    lane = lax.broadcasted_iota(jnp.int32, (seq, 128), 1)
    inside = lane % 64
    row, col = (token // grid_side, token % grid_side)
    hot = jnp.where(inside < grid_side, inside == row, inside - grid_side == col)
    hot = (hot & (inside < 2 * grid_side)).astype(NARROW)
    back = jnp.where(lane < grid_side, grid_side - 1 - lane == row, 2 * grid_side - 1 - lane == col)
    back = (back & (lane < 2 * grid_side)).astype(NARROW)
    return plain, turned, hot, back


def whole_vmem(count):
    return [pl.BlockSpec(memory_space=pltpu.VMEM)] * count


def attend_forward(qkv_rows, turned, hot, heads, size, grid_side):
    seq = qkv_rows.shape[1]
    block = min(256, seq)
    return pl.pallas_call(
        functools.partial(forward_kernel, heads, size, grid_side, block),
        out_shape=(
            jax.ShapeDtypeStruct((seq, heads * size), NARROW),
            jax.ShapeDtypeStruct((heads, seq, 128), NARROW),
            jax.ShapeDtypeStruct((heads, 1, seq), SINGLE),
        ),
        in_specs=whole_vmem(3),
        out_specs=tuple(whole_vmem(3)),
        scratch_shapes=[
            pltpu.VMEM((seq, 256), NARROW),
            pltpu.VMEM((seq, 256), NARROW),
            pltpu.VMEM((seq, 128), SINGLE),
            pltpu.VMEM((heads * size, seq), SINGLE),
        ],
        compiler_params=pltpu.CompilerParams(vmem_limit_bytes=40 << 20),
        name="attend_forward",
    )(qkv_rows, turned, hot)


def attend_backward(qkv_rows, grad_rows, bias, lse, plain, hot, back, heads, size, grid_side):
    seq = qkv_rows.shape[1]
    block = min(256, seq)
    return pl.pallas_call(
        functools.partial(backward_kernel, heads, size, grid_side, block),
        out_shape=(
            jax.ShapeDtypeStruct((3, seq, heads * size), NARROW),
            jax.ShapeDtypeStruct((128, size), SINGLE),
        ),
        in_specs=whole_vmem(7),
        out_specs=tuple(whole_vmem(2)),
        scratch_shapes=[
            pltpu.VMEM((seq, 256), NARROW),
            pltpu.VMEM((seq, 256), NARROW),
            pltpu.VMEM((seq, 256), NARROW),
            pltpu.VMEM((seq, 128), NARROW),
            pltpu.VMEM((seq, size), SINGLE),
            pltpu.VMEM((seq, size), SINGLE),
            pltpu.VMEM((seq, 128), SINGLE),
        ],
        compiler_params=pltpu.CompilerParams(vmem_limit_bytes=48 << 20),
        name="attend_backward",
    )(qkv_rows, grad_rows, bias, lse, plain, hot, back)


MESH_IDS = pl.DeviceIdType.MESH


def place_of(index, inner):
    return (index // inner, index % inner)


def greet_all(me, count, inner):
    barrier = pltpu.get_barrier_semaphore()

    def signal(step, carry):
        pl.semaphore_signal(
            barrier, inc=1, device_id=place_of((me + step) % count, inner), device_id_type=MESH_IDS
        )
        return carry

    lax.fori_loop(1, count, signal, 0)
    pl.semaphore_wait(barrier, count - 1)


def exchange_parts(me, count, inner, source, target, send_sem, recv_sem):
    def piece(step):
        other = (me + step) % count
        return pltpu.make_async_remote_copy(
            src_ref=source(other),
            dst_ref=target.at[me],
            send_sem=send_sem.at[step],
            recv_sem=recv_sem.at[step],
            device_id=place_of(other, inner),
            device_id_type=MESH_IDS,
        )

    def start(step, carry):
        piece(step).start()
        return carry

    def finish(step, carry):
        sender = (me + count - step) % count
        pltpu.make_async_remote_copy(
            src_ref=source(sender),
            dst_ref=target.at[sender],
            send_sem=send_sem.at[step],
            recv_sem=recv_sem.at[step],
            device_id=place_of(sender, inner),
            device_id_type=MESH_IDS,
        ).wait_recv()
        piece(step).wait_send()
        return carry

    return (
        lambda: lax.fori_loop(1, count, start, 0),
        lambda: lax.fori_loop(1, count, finish, 0),
    )


def exchange(*parts):
    start, finish = exchange_parts(*parts)
    start()
    finish()


def first_gather_kernel(
    outer, parts, chunks, own_ref, small_ref, all_ref, small_all_ref,
    send_sem, recv_sem, small_send, small_recv,
):
    count = outer * parts
    me = lax.axis_index("dp") * parts + lax.axis_index("tensor")
    greet_all(me, count, parts)
    start, finish = exchange_parts(
        me, count, parts, lambda other: small_ref, small_all_ref, small_send, small_recv
    )
    start()
    small_all_ref[me] = small_ref[...]
    relay_rows(parts, chunks, own_ref, all_ref, send_sem, recv_sem, lambda values, place: None)
    finish()


def small_sum_kernel(
    outer, inner, packed_ref, total_ref, all_ref, landing, send_one, recv_one, send_two, recv_two
):
    count = outer * inner
    me = lax.axis_index("dp") * inner + lax.axis_index("tensor")
    greet_all(me, count, inner)
    landing[me] = packed_ref[me]
    exchange(me, count, inner, lambda other: packed_ref.at[other], landing, send_one, recv_one)
    total = jnp.sum(landing[...], axis=0)
    total_ref[...] = total
    all_ref[me] = total
    exchange(me, count, inner, lambda other: total_ref, all_ref, send_two, recv_two)


def first_gather(own, small, outer, parts, collective_id):
    chunks = 4
    count = outer * parts
    return pl.pallas_call(
        functools.partial(first_gather_kernel, outer, parts, chunks),
        out_shape=(
            jax.ShapeDtypeStruct((parts * own.shape[0], own.shape[1]), own.dtype),
            jax.ShapeDtypeStruct((count,) + small.shape, small.dtype),
        ),
        in_specs=whole_vmem(2),
        out_specs=tuple(whole_vmem(2)),
        scratch_shapes=[pltpu.SemaphoreType.DMA((2, parts, chunks))] * 2
        + [pltpu.SemaphoreType.DMA((count,))] * 2,
        compiler_params=pltpu.CompilerParams(collective_id=collective_id, has_side_effects=True),
        name="first_gather",
    )(own, small)


def small_sum(packed, outer, inner, collective_id):
    count = outer * inner
    return pl.pallas_call(
        functools.partial(small_sum_kernel, outer, inner),
        out_shape=(
            jax.ShapeDtypeStruct(packed.shape[1:], packed.dtype),
            jax.ShapeDtypeStruct(packed.shape, packed.dtype),
        ),
        in_specs=whole_vmem(1),
        out_specs=tuple(whole_vmem(2)),
        scratch_shapes=[pltpu.VMEM(packed.shape, packed.dtype)]
        + [pltpu.SemaphoreType.DMA((count,))] * 4,
        compiler_params=pltpu.CompilerParams(collective_id=collective_id, has_side_effects=True),
        name="small_sum",
    )(packed)


def greet_line(me, parts):
    barrier = pltpu.get_barrier_semaphore()

    @pl.when(me > 0)
    def _():
        pl.semaphore_signal(barrier, inc=1, device_id={"tensor": me - 1}, device_id_type=MESH_IDS)

    @pl.when(me < parts - 1)
    def _():
        pl.semaphore_signal(barrier, inc=1, device_id={"tensor": me + 1}, device_id_type=MESH_IDS)

    @pl.when((me > 0) & (me < parts - 1))
    def _():
        pl.semaphore_wait(barrier, 2)

    @pl.when((me == 0) | (me == parts - 1))
    def _():
        pl.semaphore_wait(barrier, 1)


def gather_kernel(parts, chunks, inputs, finish_rows, own_ref, *refs):
    extra = refs[:inputs]
    all_ref = refs[inputs]
    results = refs[inputs + 1 : -2]
    send_sem, recv_sem = refs[-2:]
    greet_line(lax.axis_index("tensor"), parts)
    relay_rows(
        parts, chunks, own_ref, all_ref, send_sem, recv_sem,
        lambda values, place: finish_rows(values, place, extra, results),
    )


def relay_rows(parts, chunks, own_ref, all_ref, send_sem, recv_sem, finish_rows):
    me = lax.axis_index("tensor")
    rows = own_ref.shape[0]
    chunk = rows // chunks

    def block(shard, piece):
        return all_ref.at[pl.ds(pl.multiple_of(shard * rows + piece * chunk, chunk), chunk)]

    def outgoing(way, step, piece):
        shard = me - step if way == 0 else me + step
        source = own_ref.at[pl.ds(piece * chunk, chunk)] if step == 0 else block(shard, piece)
        return pltpu.make_async_remote_copy(
            src_ref=source,
            dst_ref=block(shard, piece),
            send_sem=send_sem.at[way, step, piece],
            recv_sem=recv_sem.at[way, step + 1, piece],
            device_id={"tensor": me + 1 if way == 0 else me - 1},
            device_id_type=MESH_IDS,
        )

    def incoming(way, step, piece):
        shard = me - step if way == 0 else me + step
        return pltpu.make_async_remote_copy(
            src_ref=block(shard, piece),
            dst_ref=block(shard, piece),
            send_sem=send_sem.at[way, step, piece],
            recv_sem=recv_sem.at[way, step, piece],
            device_id={"tensor": me - 1 if way == 0 else me + 1},
            device_id_type=MESH_IDS,
        )

    def held(way, step):
        return me - step >= 0 if way == 0 else me + step < parts

    def passes(way, step):
        return held(way, step) & ((me < parts - 1) if way == 0 else (me > 0))

    for step in range(parts):
        for piece in range(chunks):
            for way in range(2):
                if step:

                    @pl.when(held(way, step))
                    def _():
                        incoming(way, step, piece).wait_recv()

                if step < parts - 1:

                    @pl.when(passes(way, step))
                    def _():
                        outgoing(way, step, piece).start()

        if step == 0:
            mine = pl.ds(pl.multiple_of(me * rows, rows), rows)
            all_ref[mine, :] = own_ref[...]
            finish_rows(own_ref[...], mine)
        else:
            for way in range(2):

                @pl.when(held(way, step))
                def _():
                    shard = me - step if way == 0 else me + step
                    place = pl.ds(pl.multiple_of(shard * rows, rows), rows)
                    finish_rows(all_ref[place, :], place)

    for step in range(parts - 1):
        for piece in range(chunks):
            for way in range(2):

                @pl.when(passes(way, step))
                def _():
                    outgoing(way, step, piece).wait_send()


def gather_rows(own, extra, results, finish_rows, parts, collective_id, name):
    chunks = 4
    return pl.pallas_call(
        functools.partial(gather_kernel, parts, chunks, len(extra), finish_rows),
        out_shape=(jax.ShapeDtypeStruct((parts * own.shape[0], own.shape[1]), own.dtype),)
        + tuple(results),
        in_specs=whole_vmem(1 + len(extra)),
        out_specs=tuple(whole_vmem(1 + len(results))),
        scratch_shapes=[
            pltpu.SemaphoreType.DMA((2, parts, chunks)),
            pltpu.SemaphoreType.DMA((2, parts, chunks)),
        ],
        compiler_params=pltpu.CompilerParams(
            collective_id=collective_id, has_side_effects=True, vmem_limit_bytes=40 << 20
        ),
        name=name,
    )(own, *extra)


def scatter_kernel(
    parts, chunks, turned, left_ref, weight_ref, out_ref, product, landing, send_sem, recv_sem
):
    me = lax.axis_index("tensor")
    rows = out_ref.shape[0]
    chunk = rows // chunks
    greet_line(me, parts)

    def own_block(shard, piece):
        return pl.ds(pl.multiple_of(shard * rows + piece * chunk, chunk), chunk)

    def outgoing(way, far, piece, source):
        return pltpu.make_async_remote_copy(
            src_ref=source,
            dst_ref=landing.at[way, far - 1, pl.ds(piece * chunk, chunk)],
            send_sem=send_sem.at[way, far, piece],
            recv_sem=recv_sem.at[way, far - 1, piece],
            device_id={"tensor": me + 1 if way == 0 else me - 1},
            device_id_type=MESH_IDS,
        )

    def wait_landing(way, far, piece):
        spot = landing.at[way, far, pl.ds(piece * chunk, chunk)]
        pltpu.make_async_remote_copy(
            src_ref=spot,
            dst_ref=spot,
            send_sem=send_sem.at[way, far, piece],
            recv_sem=recv_sem.at[way, far, piece],
            device_id={"tensor": me - 1 if way == 0 else me + 1},
            device_id_type=MESH_IDS,
        ).wait_recv()

    def first(way):
        return me == 0 if way == 0 else me == parts - 1

    for step in range(parts):
        shard = jnp.where(me < parts // 2, parts - 1 - step, step)
        place = pl.ds(pl.multiple_of(shard * rows, rows), rows)
        total = None
        for part in range(left_ref.shape[0]):
            term = (dot_nt if turned else dot_nn)(left_ref[part, place, :], weight_ref[part])
            total = term if total is None else total + term
        product[place, :] = total.astype(NARROW)
        far = parts - 1 - step
        if far:
            for way in range(2):

                @pl.when(first(way))
                def _():
                    shard = me + far if way == 0 else me - far
                    for piece in range(chunks):
                        outgoing(way, far, piece, product.at[own_block(shard, piece)]).start()

    def relays(way, far):
        return (~first(way)) & ((me + far < parts) if way == 0 else (me - far >= 0))

    for far in range(parts - 2, 0, -1):
        for piece in range(chunks):
            for way in range(2):

                @pl.when(relays(way, far))
                def _():
                    wait_landing(way, far, piece)
                    shard = me + far if way == 0 else me - far
                    spot = (way, far, pl.ds(piece * chunk, chunk))
                    landing[spot] = (
                        landing[spot].astype(SINGLE)
                        + product[own_block(shard, piece), :].astype(SINGLE)
                    ).astype(NARROW)
                    outgoing(way, far, piece, landing.at[spot]).start()

    for piece in range(chunks):
        place = pl.ds(piece * chunk, chunk)
        out_ref[place, :] = product[own_block(me, piece), :].astype(SINGLE)
        for way in range(2):

            @pl.when(~first(way))
            def _():
                wait_landing(way, 0, piece)
                out_ref[place, :] += landing[way, 0, place].astype(SINGLE)

    for far in range(parts - 1, 0, -1):
        for piece in range(chunks):
            for way in range(2):
                shard = me + far if way == 0 else me - far

                @pl.when(first(way))
                def _():
                    outgoing(way, far, piece, product.at[own_block(shard, piece)]).wait_send()

                if far < parts - 1:

                    @pl.when(relays(way, far))
                    def _():
                        spot = landing.at[way, far, pl.ds(piece * chunk, chunk)]
                        outgoing(way, far, piece, spot).wait_send()


def scatter_rows(left, weight, turned, parts, collective_id, name):
    chunks = 4
    total_rows = left.shape[1]
    rows = total_rows // parts
    width = weight.shape[1] if turned else weight.shape[2]
    return pl.pallas_call(
        functools.partial(scatter_kernel, parts, chunks, turned),
        out_shape=jax.ShapeDtypeStruct((rows, width), SINGLE),
        in_specs=whole_vmem(2),
        out_specs=whole_vmem(1)[0],
        scratch_shapes=[
            pltpu.VMEM((total_rows, width), NARROW),
            pltpu.VMEM((2, parts - 1, rows, width), NARROW),
            pltpu.SemaphoreType.DMA((2, parts, chunks)),
            pltpu.SemaphoreType.DMA((2, parts, chunks)),
        ],
        compiler_params=pltpu.CompilerParams(
            collective_id=collective_id, has_side_effects=True, vmem_limit_bytes=40 << 20
        ),
        name=name,
    )(left, weight)


def project_rows(values, place, extra, results):
    weight_ref, bias_ref = extra
    for part in range(weight_ref.shape[0]):
        total = dot_nn(values, weight_ref[part]) + bias_ref[part]
        results[0][part, place, :] = total.astype(NARROW)


def expand_rows(values, place, extra, results):
    weight_ref, bias_ref = extra
    hidden = dot_nn(values, weight_ref[...]) + bias_ref[...]
    cumulative = 0.5 * (1.0 + lax.erf(hidden * 0.7071067811865476))
    density = 0.3989422804014327 * jnp.exp(-0.5 * hidden * hidden)
    results[0][place, :] = (hidden * cumulative).astype(NARROW)
    results[1][place, :] = cumulative + hidden * density


def context_grad_rows(values, place, extra, results):
    results[0][place, :] = dot_nt(values, extra[0][...]).astype(NARROW)


TILE = 1024


def as_tiles(vector):
    return jnp.pad(vector, (0, TILE - vector.shape[0])).reshape(8, 128)


def advance(weight, moment, average, gradient, rate_value):
    new_moment = MOMENTUM * moment + gradient
    new_weight = weight - rate_value * (gradient + MOMENTUM * new_moment)
    new_average = AVERAGING * average + (1.0 - AVERAGING) * new_weight
    return (new_weight, new_moment, new_average)


def local(
    tokens,
    cotangent,
    qkv_weight,
    out_weight,
    expand_weight,
    reduce_weight,
    gains_biases,
    rel_tables,
    qkv_moment,
    out_moment,
    expand_moment,
    reduce_moment,
    gains_moment,
    rel_moment,
    qkv_average,
    out_average,
    expand_average,
    reduce_average,
    gains_average,
    rel_average,
):
    local_seq, local_images, model_width = tokens.shape
    tensor_count = lax.axis_size("tensor")
    tensor_index = lax.axis_index("tensor")
    local_rows = local_seq * local_images
    seq_length = local_seq * tensor_count
    head_width = qkv_weight.shape[2]
    hidden_width = expand_weight.shape[1]
    head_size = rel_tables.shape[2]
    grid_side = (rel_tables.shape[1] + 1) // 2
    qkv_full = lax.all_gather(qkv_weight.astype(NARROW), "dp", axis=1, tiled=True)
    columns_full = lax.all_gather(
        jnp.concatenate([out_weight, reduce_weight]).astype(NARROW), "dp", axis=1, tiled=True
    )
    out_full, reduce_full = (columns_full[:head_width], columns_full[head_width:])
    expand_full = lax.all_gather(expand_weight.astype(NARROW), "dp", axis=0, tiled=True)
    piece = gains_biases.shape[0]
    outer = lax.axis_size("dp")
    cotangent_rows = cotangent.reshape(local_rows, model_width)
    output_grads, params_all = first_gather(
        cotangent_rows, as_tiles(gains_biases), outer, tensor_count, 0
    )
    params_all = params_all.reshape(-1, TILE)[:, :piece].reshape(-1)

    def segment(position):
        return params_all[position * model_width : (position + 1) * model_width]

    query_bias = lax.dynamic_slice_in_dim(
        params_all, 2 * model_width + tensor_index * head_width, head_width
    )
    value_bias = lax.dynamic_slice_in_dim(
        params_all, 3 * model_width + tensor_index * head_width, head_width
    )
    heads = head_width // head_size
    plain, turned, hot, back = attention_tables(rel_tables.astype(NARROW), grid_side)
    token_rows = tokens.reshape(local_rows, model_width).astype(SINGLE)
    normed_one, scaled_one, inverse_one = normalize(token_rows, segment(0), segment(1))
    qkv_bias = jnp.stack([query_bias, jnp.zeros((head_width,), SINGLE), value_bias])
    gathered_one, qkv_rows = gather_rows(
        normed_one.astype(NARROW),
        (qkv_full, qkv_bias[:, None]),
        (jax.ShapeDtypeStruct((3, seq_length, head_width), NARROW),),
        project_rows, tensor_count, 2, "gather_project",
    )
    context_rows, bias_wide, logsums = attend_forward(
        qkv_rows, turned, hot, heads, head_size, grid_side
    )
    attn_sum = scatter_rows(context_rows[None], out_full[None], False, tensor_count, 3, "scatter_out")
    mid_rows = token_rows + (attn_sum + segment(4))
    normed_two, scaled_two, inverse_two = normalize(mid_rows, segment(5), segment(6))
    normed_two_low = normed_two.astype(NARROW)
    expand_bias = lax.dynamic_slice_in_dim(
        params_all, 8 * model_width + tensor_index * hidden_width, hidden_width
    )
    gathered_two, hidden_low, hidden_slope = gather_rows(
        normed_two_low,
        (expand_full, expand_bias[None]),
        (
            jax.ShapeDtypeStruct((seq_length, hidden_width), NARROW),
            jax.ShapeDtypeStruct((seq_length, hidden_width), SINGLE),
        ),
        expand_rows, tensor_count, 4, "gather_expand",
    )
    mlp_part = jnp.dot(hidden_low, reduce_full, preferred_element_type=SINGLE).astype(NARROW)
    grad_block = cotangent_rows.astype(SINGLE)
    grad_reduce_bias = jnp.sum(grad_block, axis=0)
    shard_rows = output_grads
    part_hidden = contract_cols(shard_rows, reduce_full)
    grad_hidden = part_hidden
    grad_hidden, grad_reduce = (grad_hidden, contract_rows(hidden_low, shard_rows))
    grad_pre = (grad_hidden * hidden_slope).astype(NARROW)
    grad_expand = contract_rows(gathered_two, grad_pre)
    grad_expand_bias = jnp.sum(grad_pre, axis=0, dtype=SINGLE)
    expand_bias_full = lax.dynamic_update_slice_in_dim(
        jnp.zeros((hidden_width * tensor_count,), SINGLE),
        grad_expand_bias,
        tensor_index * hidden_width,
        0,
    )
    grad_reduce, grad_expand = (grad_reduce.astype(NARROW), grad_expand.astype(NARROW))
    grad_pre, grad_reduce, mlp_part, grad_expand = lax.optimization_barrier(
        (grad_pre, grad_reduce, mlp_part, grad_expand)
    )
    reduce_sum = lax.psum_scatter(grad_reduce, "dp", scatter_dimension=1, tiled=True)
    mlp_sum = lax.psum_scatter(mlp_part, "tensor", scatter_dimension=0, tiled=True)
    expand_sum = lax.psum_scatter(grad_expand, "dp", scatter_dimension=0, tiled=True)
    grad_normed_two = scatter_rows(
        grad_pre[None], expand_full[None], True, tensor_count, 5, "scatter_expand"
    )
    grad_mid_norm, grad_gain_two, grad_shift_two = normalize_back(
        grad_normed_two, scaled_two, inverse_two, segment(5)
    )
    grad_mid = grad_block + grad_mid_norm
    grad_attn_low = grad_mid.astype(NARROW)
    grad_out_bias = jnp.sum(grad_attn_low, axis=0, dtype=SINGLE)
    shard_rows, grad_context = gather_rows(
        grad_attn_low,
        (out_full,),
        (jax.ShapeDtypeStruct((seq_length, head_width), NARROW),),
        context_grad_rows, tensor_count, 6, "gather_context",
    )
    grad_out = contract_rows(context_rows, shard_rows).astype(NARROW)
    late_rows = lax.optimization_barrier((mid_rows, shard_rows))[0]
    block_rows = late_rows + (mlp_sum.astype(SINGLE) + segment(7))
    block_out = block_rows.astype(NARROW).reshape(tokens.shape)
    grad_context, grad_out, reduce_sum = lax.optimization_barrier(
        (grad_context, grad_out, reduce_sum)
    )
    grad_qkv_rows, grad_tables = attend_backward(
        qkv_rows, grad_context, bias_wide, logsums, plain, hot, back,
        heads, head_size, grid_side,
    )
    grad_query_bias = jnp.sum(grad_qkv_rows[0], axis=0, dtype=SINGLE)
    grad_value_bias = jnp.sum(grad_qkv_rows[2], axis=0, dtype=SINGLE)
    grad_qkv = jnp.concatenate(
        [contract_rows(gathered_one, grad_qkv_rows[part]).astype(NARROW) for part in range(3)],
        axis=1,
    )
    grad_qkv_rows, grad_qkv, block_out = lax.optimization_barrier(
        (grad_qkv_rows, grad_qkv, block_out)
    )
    grad_normed_one = scatter_rows(
        grad_qkv_rows, qkv_full, True, tensor_count, 7, "scatter_qkv"
    )
    grad_token_norm, grad_gain_one, grad_shift_one = normalize_back(
        grad_normed_one, scaled_one, inverse_one, segment(0)
    )
    token_grad = (grad_mid + grad_token_norm).reshape(tokens.shape)
    rel_own = grad_tables.reshape(2, 64, head_size)[:, : rel_tables.shape[1]]
    width_zeros = jnp.zeros((model_width,), SINGLE)
    grad_small = jnp.concatenate(
        [
            grad_gain_one,
            grad_shift_one,
            lax.dynamic_update_slice_in_dim(
                width_zeros, grad_query_bias, tensor_index * head_width, 0
            ),
            lax.dynamic_update_slice_in_dim(
                width_zeros, grad_value_bias, tensor_index * head_width, 0
            ),
            grad_out_bias,
            grad_gain_two,
            grad_shift_two,
            grad_reduce_bias,
            expand_bias_full,
        ]
    )
    devices = lax.axis_size("dp") * tensor_count
    rel_flat = rel_own.reshape(-1)
    rel_piece = -(-rel_flat.shape[0] // devices)
    rel_flat = jnp.pad(rel_flat, (0, rel_piece * devices - rel_flat.shape[0]))
    packed = jnp.concatenate(
        [grad_small.reshape(devices, piece), rel_flat.reshape(devices, rel_piece)], axis=1
    )
    own_sum, rel_grad = small_sum(jax.vmap(as_tiles)(packed), outer, tensor_count, 1)
    gains_grad = own_sum.reshape(-1)[:piece]
    rel_grad = rel_grad.reshape(devices, TILE)[:, piece : piece + rel_piece].reshape(-1)
    rel_grad = rel_grad[: rel_tables.size].reshape(rel_tables.shape)
    qkv_grad, out_grad, expand_grad, reduce_grad = (
        lax.psum_scatter(grad_qkv, "dp", scatter_dimension=0, tiled=True)
        .astype(SINGLE)
        .reshape(-1, 3, head_width)
        .transpose(1, 0, 2),
        lax.psum_scatter(grad_out.astype(NARROW), "dp", scatter_dimension=1, tiled=True).astype(SINGLE),
        expand_sum.astype(SINGLE),
        reduce_sum.astype(SINGLE),
    )
    reduce_moment = lax.optimization_barrier((reduce_moment, grad_normed_two))[0]
    expand_moment = lax.optimization_barrier((expand_moment, grad_tables))[0]
    out_moment = lax.optimization_barrier((out_moment, grad_normed_one))[0]
    new_qkv, moment_qkv, average_qkv = advance(
        qkv_weight, qkv_moment, qkv_average, qkv_grad, RATE_MAIN
    )
    new_out, moment_out, average_out = advance(
        out_weight, out_moment, out_average, out_grad, RATE_MAIN
    )
    new_expand, moment_expand, average_expand = advance(
        expand_weight, expand_moment, expand_average, expand_grad, RATE_MAIN
    )
    new_reduce, moment_reduce, average_reduce = advance(
        reduce_weight, reduce_moment, reduce_average, reduce_grad, RATE_MAIN
    )
    new_gains, moment_gains, average_gains = advance(
        gains_biases, gains_moment, gains_average, gains_grad, RATE_MAIN
    )
    new_rel, moment_rel, average_rel = advance(
        rel_tables, rel_moment, rel_average, rel_grad, RATE_TABLES
    )
    return (
        block_out,
        token_grad,
        qkv_grad,
        out_grad,
        expand_grad,
        reduce_grad,
        gains_grad,
        rel_grad,
        new_qkv,
        new_out,
        new_expand,
        new_reduce,
        new_gains,
        new_rel,
        moment_qkv,
        moment_out,
        moment_expand,
        moment_reduce,
        moment_gains,
        moment_rel,
        average_qkv,
        average_out,
        average_expand,
        average_reduce,
        average_gains,
        average_rel,
    )


def solution(mesh):
    placed = (
        P("tensor", "dp", None),
        P("tensor", "dp", None),
        P(None, "dp", "tensor"),
        P("tensor", "dp"),
        P("dp", "tensor"),
        P("tensor", "dp"),
        P(("dp", "tensor")),
        P(),
        P(None, "dp", "tensor"),
        P("tensor", "dp"),
        P("dp", "tensor"),
        P("tensor", "dp"),
        P(("dp", "tensor")),
        P(),
        P(None, "dp", "tensor"),
        P("tensor", "dp"),
        P("dp", "tensor"),
        P("tensor", "dp"),
        P(("dp", "tensor")),
        P(),
    )
    return jax.shard_map(
        local,
        mesh=mesh,
        in_specs=placed,
        out_specs=(
            P("tensor", "dp", None),
            P("tensor", "dp", None),
            P(None, "dp", "tensor"),
            P("tensor", "dp"),
            P("dp", "tensor"),
            P("tensor", "dp"),
            P(("dp", "tensor")),
            P(),
            P(None, "dp", "tensor"),
            P("tensor", "dp"),
            P("dp", "tensor"),
            P("tensor", "dp"),
            P(("dp", "tensor")),
            P(),
            P(None, "dp", "tensor"),
            P("tensor", "dp"),
            P("dp", "tensor"),
            P("tensor", "dp"),
            P(("dp", "tensor")),
            P(),
            P(None, "dp", "tensor"),
            P("tensor", "dp"),
            P("dp", "tensor"),
            P("tensor", "dp"),
            P(("dp", "tensor")),
            P(),
        ),
        check_vma=False,
    )
```

```python
import functools
import jax
import jax.numpy as jnp
from jax import lax
from jax.experimental import pallas as pl
from jax.experimental.pallas import tpu as pltpu
from jax.sharding import PartitionSpec as P

EPSILON = 1e-06
MOMENTUM = 0.5
AVERAGING = 0.5
RATE_MAIN = 0.0003
RATE_TABLES = 0.01
NARROW = jnp.bfloat16
SINGLE = jnp.float32


def normalize(values, gain_row, shift_row):
    center = values - jnp.mean(values, axis=-1, keepdims=True)
    inverse = lax.rsqrt(jnp.mean(center * center, axis=-1, keepdims=True) + EPSILON)
    scaled = center * inverse
    return (scaled * gain_row + shift_row, scaled, inverse)


def normalize_back(grad_output, scaled, inverse, gain_row):
    grad_scaled = grad_output * gain_row
    mean_plain = jnp.mean(grad_scaled, axis=-1, keepdims=True)
    mean_cross = jnp.mean(grad_scaled * scaled, axis=-1, keepdims=True)
    grad_values = inverse * (grad_scaled - mean_plain - scaled * mean_cross)
    return (grad_values, jnp.sum(grad_output * scaled, axis=0), jnp.sum(grad_output, axis=0))


def gelu_slope(values):
    cumulative = 0.5 * (1.0 + lax.erf(values * 0.7071067811865476))
    density = 0.3989422804014327 * jnp.exp(-0.5 * values * values)
    return cumulative + values * density


def contract_rows(left_side, right_side):
    return lax.dot_general(
        left_side, right_side, (((0,), (0,)), ((), ())), preferred_element_type=SINGLE
    )


def contract_cols(left_side, right_side):
    return lax.dot_general(
        left_side, right_side, (((1,), (1,)), ((), ())), preferred_element_type=SINGLE
    )


def dot_nt(left, right):
    return lax.dot_general(left, right, (((1,), (1,)), ((), ())), preferred_element_type=SINGLE)


def dot_tn(left, right):
    return lax.dot_general(left, right, (((0,), (0,)), ((), ())), preferred_element_type=SINGLE)


def dot_nn(left, right):
    return lax.dot_general(left, right, (((1,), (0,)), ((), ())), preferred_element_type=SINGLE)


def forward_kernel(
    heads, size, grid_side, block, qkv_ref, table_ref, hot_ref,
    out_ref, bias_ref, lse_ref, query_ext, key_ext, bias_wide, context_t,
):
    seq = qkv_ref.shape[1]
    scale = size ** (-0.5)
    lane = lax.broadcasted_iota(jnp.int32, (grid_side, 128), 1)
    query_ext[:, 0:128] = jnp.zeros((seq, 128), NARROW)
    key_ext[:, 0:128] = jnp.zeros((seq, 128), NARROW)
    key_ext[:, 128:256] = hot_ref[...]
    for head in range(heads):
        low = head * size
        query = qkv_ref[0, :, low : low + size]
        value = qkv_ref[2, :, low : low + size]
        query_ext[:, 0:size] = query
        key_ext[:, 0:size] = qkv_ref[1, :, low : low + size]
        bias_wide[...] = dot_nt(query, table_ref[...])
        for row in range(grid_side):
            rows = pl.ds(row * grid_side, grid_side)
            group = bias_wide[rows, :]
            part_row = pltpu.roll(group, (128 - grid_side + 1 + row) % 128, 1)
            part_col = pltpu.roll(group, 65 - 32 + grid_side, 1, stride=1, stride_axis=0)
            both = jnp.where(
                lane < grid_side, part_row, jnp.where(lane < 2 * grid_side, part_col, 0.0)
            ) * (size ** 0.5)
            high = both.astype(NARROW).astype(SINGLE)
            rest = pltpu.roll(both - high, 64, 1)
            mixed = jnp.where(lane < 64, high, rest).astype(NARROW)
            query_ext[rows, 128:256] = mixed
        bias_ref[head] = query_ext[:, 128:256]
        for start in range(0, seq, block):
            scores = dot_nt(key_ext[...], query_ext[start : start + block, :])
            highest = jnp.max(scores, axis=0, keepdims=True)
            powers = jnp.exp((scores - highest) * scale)
            total = jnp.sum(powers, axis=0, keepdims=True)
            weights = (powers * (1.0 / total)).astype(NARROW)
            lse_ref[head, :, start : start + block] = highest * scale + jnp.log(total)
            context_t[low : low + size, start : start + block] = dot_tn(value, weights)
    out_ref[...] = context_t[...].T.astype(NARROW)


def backward_kernel(
    heads, size, grid_side, block, qkv_ref, grad_ref, bias_ref, lse_ref, table_ref, hot_ref, rev_ref,
    out_ref, rel_ref, query_ext, key_ext, key_rev, spread, grad_keys, grad_values, grad_query,
):
    seq = qkv_ref.shape[1]
    scale = size ** (-0.5)
    lane = lax.broadcasted_iota(jnp.int32, (grid_side, 128), 1)
    query_ext[:, 0:128] = jnp.zeros((seq, 128), NARROW)
    key_ext[:, 0:128] = jnp.zeros((seq, 128), NARROW)
    key_ext[:, 128:256] = hot_ref[...]
    key_rev[:, 0:128] = jnp.zeros((seq, 128), NARROW)
    key_rev[:, 128:256] = rev_ref[...]
    rel_total = jnp.zeros(rel_ref.shape, SINGLE)
    for head in range(heads):
        low = head * size
        query = qkv_ref[0, :, low : low + size]
        key = qkv_ref[1, :, low : low + size]
        value = qkv_ref[2, :, low : low + size]
        grad = grad_ref[:, low : low + size]
        query_ext[:, 0:size] = query
        query_ext[:, 128:256] = bias_ref[head]
        key_ext[:, 0:size] = key
        key_rev[:, 0:size] = key
        for start in range(0, seq, block):
            part = slice(start, start + block)
            scores = dot_nt(key_ext[...], query_ext[part, :])
            soft = jnp.exp(scores * scale - lse_ref[head, :, part])
            grad_part = grad[part]
            grad_soft = dot_nt(value, grad_part)
            inner = jnp.sum(soft * grad_soft, axis=0, keepdims=True)
            grad_scores = (soft * (grad_soft - inner)).astype(NARROW)
            add_values = dot_nn(soft.astype(NARROW), grad_part)
            add_keys = dot_nn(grad_scores, query[part])
            if start == 0:
                grad_values[...] = add_values
                grad_keys[...] = add_keys
            else:
                grad_values[...] += add_values
                grad_keys[...] += add_keys
            turned = dot_tn(key_rev[...], grad_scores).T
            grad_query[part, :] = turned[:, 0:128]
            sums = turned[:, 128:256].astype(NARROW).astype(SINGLE)
            for inside in range(block // grid_side):
                row = start // grid_side + inside
                group = sums[inside * grid_side : (inside + 1) * grid_side]
                part_row = jnp.where(lane < grid_side, group, 0.0)
                part_col = jnp.where((lane >= grid_side) & (lane < 2 * grid_side), group, 0.0)
                if row:
                    part_row = pltpu.roll(part_row, row, 1)
                part_col = pltpu.roll(part_col, 64 - grid_side, 1, stride=1, stride_axis=0)
                spread[row * grid_side : (row + 1) * grid_side, :] = (part_row + part_col).astype(NARROW)
        total_query = grad_query[:, 0:size] * scale + dot_nn(spread[...], table_ref[...])
        out_ref[0, :, low : low + size] = total_query.astype(NARROW)
        out_ref[1, :, low : low + size] = (grad_keys[...] * scale).astype(NARROW)
        out_ref[2, :, low : low + size] = grad_values[...].astype(NARROW)
        rel_total = rel_total + dot_tn(spread[...], query)
    rel_ref[...] = rel_total


def attention_tables(rel_low, grid_side):
    offsets = rel_low.shape[1]
    pad = ((0, 0), (0, 64 - offsets), (0, 0))
    plain = jnp.pad(rel_low, pad).reshape(128, -1)
    turned = jnp.pad(rel_low[:, ::-1], pad).reshape(128, -1)
    seq = grid_side * grid_side
    token = lax.broadcasted_iota(jnp.int32, (seq, 128), 0)
    lane = lax.broadcasted_iota(jnp.int32, (seq, 128), 1)
    inside = lane % 64
    row, col = (token // grid_side, token % grid_side)
    hot = jnp.where(inside < grid_side, inside == row, inside - grid_side == col)
    hot = (hot & (inside < 2 * grid_side)).astype(NARROW)
    back = jnp.where(lane < grid_side, grid_side - 1 - lane == row, 2 * grid_side - 1 - lane == col)
    back = (back & (lane < 2 * grid_side)).astype(NARROW)
    return plain, turned, hot, back


def whole_vmem(count):
    return [pl.BlockSpec(memory_space=pltpu.VMEM)] * count


def attend_forward(qkv_rows, turned, hot, heads, size, grid_side):
    seq = qkv_rows.shape[1]
    block = min(256, seq)
    return pl.pallas_call(
        functools.partial(forward_kernel, heads, size, grid_side, block),
        out_shape=(
            jax.ShapeDtypeStruct((seq, heads * size), NARROW),
            jax.ShapeDtypeStruct((heads, seq, 128), NARROW),
            jax.ShapeDtypeStruct((heads, 1, seq), SINGLE),
        ),
        in_specs=whole_vmem(3),
        out_specs=tuple(whole_vmem(3)),
        scratch_shapes=[
            pltpu.VMEM((seq, 256), NARROW),
            pltpu.VMEM((seq, 256), NARROW),
            pltpu.VMEM((seq, 128), SINGLE),
            pltpu.VMEM((heads * size, seq), SINGLE),
        ],
        compiler_params=pltpu.CompilerParams(vmem_limit_bytes=40 << 20),
        name="attend_forward",
    )(qkv_rows, turned, hot)


def attend_backward(qkv_rows, grad_rows, bias, lse, plain, hot, back, heads, size, grid_side):
    seq = qkv_rows.shape[1]
    block = min(256, seq)
    return pl.pallas_call(
        functools.partial(backward_kernel, heads, size, grid_side, block),
        out_shape=(
            jax.ShapeDtypeStruct((3, seq, heads * size), NARROW),
            jax.ShapeDtypeStruct((128, size), SINGLE),
        ),
        in_specs=whole_vmem(7),
        out_specs=tuple(whole_vmem(2)),
        scratch_shapes=[
            pltpu.VMEM((seq, 256), NARROW),
            pltpu.VMEM((seq, 256), NARROW),
            pltpu.VMEM((seq, 256), NARROW),
            pltpu.VMEM((seq, 128), NARROW),
            pltpu.VMEM((seq, size), SINGLE),
            pltpu.VMEM((seq, size), SINGLE),
            pltpu.VMEM((seq, 128), SINGLE),
        ],
        compiler_params=pltpu.CompilerParams(vmem_limit_bytes=48 << 20),
        name="attend_backward",
    )(qkv_rows, grad_rows, bias, lse, plain, hot, back)


MESH_IDS = pl.DeviceIdType.MESH


def place_of(index, inner):
    return (index // inner, index % inner)


def greet_all(me, count, inner):
    barrier = pltpu.get_barrier_semaphore()

    def signal(step, carry):
        pl.semaphore_signal(
            barrier, inc=1, device_id=place_of((me + step) % count, inner), device_id_type=MESH_IDS
        )
        return carry

    lax.fori_loop(1, count, signal, 0)
    pl.semaphore_wait(barrier, count - 1)


def exchange_parts(me, count, inner, source, target, send_sem, recv_sem):
    def piece(step):
        other = (me + step) % count
        return pltpu.make_async_remote_copy(
            src_ref=source(other),
            dst_ref=target.at[me],
            send_sem=send_sem.at[step],
            recv_sem=recv_sem.at[step],
            device_id=place_of(other, inner),
            device_id_type=MESH_IDS,
        )

    def start(step, carry):
        piece(step).start()
        return carry

    def finish(step, carry):
        sender = (me + count - step) % count
        pltpu.make_async_remote_copy(
            src_ref=source(sender),
            dst_ref=target.at[sender],
            send_sem=send_sem.at[step],
            recv_sem=recv_sem.at[step],
            device_id=place_of(sender, inner),
            device_id_type=MESH_IDS,
        ).wait_recv()
        piece(step).wait_send()
        return carry

    return (
        lambda: lax.fori_loop(1, count, start, 0),
        lambda: lax.fori_loop(1, count, finish, 0),
    )


def exchange(*parts):
    start, finish = exchange_parts(*parts)
    start()
    finish()


def first_gather_kernel(
    outer, parts, chunks, own_ref, small_ref, all_ref, small_all_ref,
    send_sem, recv_sem, small_send, small_recv,
):
    count = outer * parts
    me = lax.axis_index("dp") * parts + lax.axis_index("tensor")
    greet_all(me, count, parts)
    start, finish = exchange_parts(
        me, count, parts, lambda other: small_ref, small_all_ref, small_send, small_recv
    )
    start()
    small_all_ref[me] = small_ref[...]
    relay_rows(parts, chunks, own_ref, all_ref, send_sem, recv_sem, lambda values, place: None)
    finish()


def small_sum_kernel(
    outer, inner, packed_ref, total_ref, all_ref, landing, send_one, recv_one, send_two, recv_two
):
    count = outer * inner
    me = lax.axis_index("dp") * inner + lax.axis_index("tensor")
    greet_all(me, count, inner)
    landing[me] = packed_ref[me]
    exchange(me, count, inner, lambda other: packed_ref.at[other], landing, send_one, recv_one)
    total = jnp.sum(landing[...], axis=0)
    total_ref[...] = total
    all_ref[me] = total
    exchange(me, count, inner, lambda other: total_ref, all_ref, send_two, recv_two)


def first_gather(own, small, outer, parts, collective_id):
    chunks = 4
    count = outer * parts
    return pl.pallas_call(
        functools.partial(first_gather_kernel, outer, parts, chunks),
        out_shape=(
            jax.ShapeDtypeStruct((parts * own.shape[0], own.shape[1]), own.dtype),
            jax.ShapeDtypeStruct((count,) + small.shape, small.dtype),
        ),
        in_specs=whole_vmem(2),
        out_specs=tuple(whole_vmem(2)),
        scratch_shapes=[pltpu.SemaphoreType.DMA((2, parts, chunks))] * 2
        + [pltpu.SemaphoreType.DMA((count,))] * 2,
        compiler_params=pltpu.CompilerParams(collective_id=collective_id, has_side_effects=True),
        name="first_gather",
    )(own, small)


def small_sum(packed, outer, inner, collective_id):
    count = outer * inner
    return pl.pallas_call(
        functools.partial(small_sum_kernel, outer, inner),
        out_shape=(
            jax.ShapeDtypeStruct(packed.shape[1:], packed.dtype),
            jax.ShapeDtypeStruct(packed.shape, packed.dtype),
        ),
        in_specs=whole_vmem(1),
        out_specs=tuple(whole_vmem(2)),
        scratch_shapes=[pltpu.VMEM(packed.shape, packed.dtype)]
        + [pltpu.SemaphoreType.DMA((count,))] * 4,
        compiler_params=pltpu.CompilerParams(collective_id=collective_id, has_side_effects=True),
        name="small_sum",
    )(packed)


def greet_line(me, parts):
    barrier = pltpu.get_barrier_semaphore()

    @pl.when(me > 0)
    def _():
        pl.semaphore_signal(barrier, inc=1, device_id={"tensor": me - 1}, device_id_type=MESH_IDS)

    @pl.when(me < parts - 1)
    def _():
        pl.semaphore_signal(barrier, inc=1, device_id={"tensor": me + 1}, device_id_type=MESH_IDS)

    @pl.when((me > 0) & (me < parts - 1))
    def _():
        pl.semaphore_wait(barrier, 2)

    @pl.when((me == 0) | (me == parts - 1))
    def _():
        pl.semaphore_wait(barrier, 1)


def gather_kernel(parts, chunks, inputs, finish_rows, own_ref, *refs):
    extra = refs[:inputs]
    all_ref = refs[inputs]
    results = refs[inputs + 1 : -2]
    send_sem, recv_sem = refs[-2:]
    greet_line(lax.axis_index("tensor"), parts)
    relay_rows(
        parts, chunks, own_ref, all_ref, send_sem, recv_sem,
        lambda values, place: finish_rows(values, place, extra, results),
    )


def relay_rows(parts, chunks, own_ref, all_ref, send_sem, recv_sem, finish_rows):
    me = lax.axis_index("tensor")
    rows = own_ref.shape[0]
    chunk = rows // chunks

    def block(shard, piece):
        return all_ref.at[pl.ds(pl.multiple_of(shard * rows + piece * chunk, chunk), chunk)]

    def outgoing(way, step, piece):
        shard = me - step if way == 0 else me + step
        source = own_ref.at[pl.ds(piece * chunk, chunk)] if step == 0 else block(shard, piece)
        return pltpu.make_async_remote_copy(
            src_ref=source,
            dst_ref=block(shard, piece),
            send_sem=send_sem.at[way, step, piece],
            recv_sem=recv_sem.at[way, step + 1, piece],
            device_id={"tensor": me + 1 if way == 0 else me - 1},
            device_id_type=MESH_IDS,
        )

    def incoming(way, step, piece):
        shard = me - step if way == 0 else me + step
        return pltpu.make_async_remote_copy(
            src_ref=block(shard, piece),
            dst_ref=block(shard, piece),
            send_sem=send_sem.at[way, step, piece],
            recv_sem=recv_sem.at[way, step, piece],
            device_id={"tensor": me - 1 if way == 0 else me + 1},
            device_id_type=MESH_IDS,
        )

    def held(way, step):
        return me - step >= 0 if way == 0 else me + step < parts

    def passes(way, step):
        return held(way, step) & ((me < parts - 1) if way == 0 else (me > 0))

    for step in range(parts):
        for piece in range(chunks):
            for way in range(2):
                if step:

                    @pl.when(held(way, step))
                    def _():
                        incoming(way, step, piece).wait_recv()

                if step < parts - 1:

                    @pl.when(passes(way, step))
                    def _():
                        outgoing(way, step, piece).start()

        if step == 0:
            mine = pl.ds(pl.multiple_of(me * rows, rows), rows)
            all_ref[mine, :] = own_ref[...]
            finish_rows(own_ref[...], mine)
        else:
            for way in range(2):

                @pl.when(held(way, step))
                def _():
                    shard = me - step if way == 0 else me + step
                    place = pl.ds(pl.multiple_of(shard * rows, rows), rows)
                    finish_rows(all_ref[place, :], place)

    for step in range(parts - 1):
        for piece in range(chunks):
            for way in range(2):

                @pl.when(passes(way, step))
                def _():
                    outgoing(way, step, piece).wait_send()


def gather_rows(own, extra, results, finish_rows, parts, collective_id, name):
    chunks = 4
    return pl.pallas_call(
        functools.partial(gather_kernel, parts, chunks, len(extra), finish_rows),
        out_shape=(jax.ShapeDtypeStruct((parts * own.shape[0], own.shape[1]), own.dtype),)
        + tuple(results),
        in_specs=whole_vmem(1 + len(extra)),
        out_specs=tuple(whole_vmem(1 + len(results))),
        scratch_shapes=[
            pltpu.SemaphoreType.DMA((2, parts, chunks)),
            pltpu.SemaphoreType.DMA((2, parts, chunks)),
        ],
        compiler_params=pltpu.CompilerParams(
            collective_id=collective_id, has_side_effects=True, vmem_limit_bytes=40 << 20
        ),
        name=name,
    )(own, *extra)


def scatter_kernel(
    parts, chunks, turned, left_ref, weight_ref, out_ref, product, landing, send_sem, recv_sem
):
    me = lax.axis_index("tensor")
    rows = out_ref.shape[0]
    chunk = rows // chunks
    greet_line(me, parts)

    def own_block(shard, piece):
        return pl.ds(pl.multiple_of(shard * rows + piece * chunk, chunk), chunk)

    def outgoing(way, far, piece, source):
        return pltpu.make_async_remote_copy(
            src_ref=source,
            dst_ref=landing.at[way, far - 1, pl.ds(piece * chunk, chunk)],
            send_sem=send_sem.at[way, far, piece],
            recv_sem=recv_sem.at[way, far - 1, piece],
            device_id={"tensor": me + 1 if way == 0 else me - 1},
            device_id_type=MESH_IDS,
        )

    def wait_landing(way, far, piece):
        spot = landing.at[way, far, pl.ds(piece * chunk, chunk)]
        pltpu.make_async_remote_copy(
            src_ref=spot,
            dst_ref=spot,
            send_sem=send_sem.at[way, far, piece],
            recv_sem=recv_sem.at[way, far, piece],
            device_id={"tensor": me - 1 if way == 0 else me + 1},
            device_id_type=MESH_IDS,
        ).wait_recv()

    def first(way):
        return me == 0 if way == 0 else me == parts - 1

    for step in range(parts):
        shard = jnp.where(me < parts // 2, parts - 1 - step, step)
        place = pl.ds(pl.multiple_of(shard * rows, rows), rows)
        total = None
        for part in range(left_ref.shape[0]):
            term = (dot_nt if turned else dot_nn)(left_ref[part, place, :], weight_ref[part])
            total = term if total is None else total + term
        product[place, :] = total.astype(NARROW)
        far = parts - 1 - step
        if far:
            for way in range(2):

                @pl.when(first(way))
                def _():
                    shard = me + far if way == 0 else me - far
                    for piece in range(chunks):
                        outgoing(way, far, piece, product.at[own_block(shard, piece)]).start()

    def relays(way, far):
        return (~first(way)) & ((me + far < parts) if way == 0 else (me - far >= 0))

    for far in range(parts - 2, 0, -1):
        for piece in range(chunks):
            for way in range(2):

                @pl.when(relays(way, far))
                def _():
                    wait_landing(way, far, piece)
                    shard = me + far if way == 0 else me - far
                    spot = (way, far, pl.ds(piece * chunk, chunk))
                    landing[spot] = (
                        landing[spot].astype(SINGLE)
                        + product[own_block(shard, piece), :].astype(SINGLE)
                    ).astype(NARROW)
                    outgoing(way, far, piece, landing.at[spot]).start()

    for piece in range(chunks):
        place = pl.ds(piece * chunk, chunk)
        out_ref[place, :] = product[own_block(me, piece), :].astype(SINGLE)
        for way in range(2):

            @pl.when(~first(way))
            def _():
                wait_landing(way, 0, piece)
                out_ref[place, :] += landing[way, 0, place].astype(SINGLE)

    for far in range(parts - 1, 0, -1):
        for piece in range(chunks):
            for way in range(2):
                shard = me + far if way == 0 else me - far

                @pl.when(first(way))
                def _():
                    outgoing(way, far, piece, product.at[own_block(shard, piece)]).wait_send()

                if far < parts - 1:

                    @pl.when(relays(way, far))
                    def _():
                        spot = landing.at[way, far, pl.ds(piece * chunk, chunk)]
                        outgoing(way, far, piece, spot).wait_send()


def scatter_rows(left, weight, turned, parts, collective_id, name):
    chunks = 4
    total_rows = left.shape[1]
    rows = total_rows // parts
    width = weight.shape[1] if turned else weight.shape[2]
    return pl.pallas_call(
        functools.partial(scatter_kernel, parts, chunks, turned),
        out_shape=jax.ShapeDtypeStruct((rows, width), SINGLE),
        in_specs=whole_vmem(2),
        out_specs=whole_vmem(1)[0],
        scratch_shapes=[
            pltpu.VMEM((total_rows, width), NARROW),
            pltpu.VMEM((2, parts - 1, rows, width), NARROW),
            pltpu.SemaphoreType.DMA((2, parts, chunks)),
            pltpu.SemaphoreType.DMA((2, parts, chunks)),
        ],
        compiler_params=pltpu.CompilerParams(
            collective_id=collective_id, has_side_effects=True, vmem_limit_bytes=40 << 20
        ),
        name=name,
    )(left, weight)


def project_rows(values, place, extra, results):
    weight_ref, bias_ref = extra
    for part in range(weight_ref.shape[0]):
        total = dot_nn(values, weight_ref[part]) + bias_ref[part]
        results[0][part, place, :] = total.astype(NARROW)


def expand_rows(values, place, extra, results):
    weight_ref, bias_ref = extra
    hidden = dot_nn(values, weight_ref[...]) + bias_ref[...]
    cumulative = 0.5 * (1.0 + lax.erf(hidden * 0.7071067811865476))
    density = 0.3989422804014327 * jnp.exp(-0.5 * hidden * hidden)
    results[0][place, :] = (hidden * cumulative).astype(NARROW)
    results[1][place, :] = cumulative + hidden * density


def context_grad_rows(values, place, extra, results):
    results[0][place, :] = dot_nt(values, extra[0][...]).astype(NARROW)


TILE = 1024


def as_tiles(vector):
    return jnp.pad(vector, (0, TILE - vector.shape[0])).reshape(8, 128)


def advance(weight, moment, average, gradient, rate_value):
    new_moment = MOMENTUM * moment + gradient
    new_weight = weight - rate_value * (gradient + MOMENTUM * new_moment)
    new_average = AVERAGING * average + (1.0 - AVERAGING) * new_weight
    return (new_weight, new_moment, new_average)


def local(
    tokens,
    cotangent,
    qkv_weight,
    out_weight,
    expand_weight,
    reduce_weight,
    gains_biases,
    rel_tables,
    qkv_moment,
    out_moment,
    expand_moment,
    reduce_moment,
    gains_moment,
    rel_moment,
    qkv_average,
    out_average,
    expand_average,
    reduce_average,
    gains_average,
    rel_average,
):
    local_seq, local_images, model_width = tokens.shape
    tensor_count = lax.axis_size("tensor")
    tensor_index = lax.axis_index("tensor")
    local_rows = local_seq * local_images
    seq_length = local_seq * tensor_count
    head_width = qkv_weight.shape[2]
    hidden_width = expand_weight.shape[1]
    head_size = rel_tables.shape[2]
    grid_side = (rel_tables.shape[1] + 1) // 2
    qkv_full = lax.all_gather(qkv_weight.astype(NARROW), "dp", axis=1, tiled=True)
    columns_full = lax.all_gather(
        jnp.concatenate([out_weight, reduce_weight]).astype(NARROW), "dp", axis=1, tiled=True
    )
    out_full, reduce_full = (columns_full[:head_width], columns_full[head_width:])
    expand_full = lax.all_gather(expand_weight.astype(NARROW), "dp", axis=0, tiled=True)
    piece = gains_biases.shape[0]
    outer = lax.axis_size("dp")
    cotangent_rows = cotangent.reshape(local_rows, model_width)
    output_grads, params_all = first_gather(
        cotangent_rows, as_tiles(gains_biases), outer, tensor_count, 0
    )
    params_all = params_all.reshape(-1, TILE)[:, :piece].reshape(-1)

    def segment(position):
        return params_all[position * model_width : (position + 1) * model_width]

    query_bias = lax.dynamic_slice_in_dim(
        params_all, 2 * model_width + tensor_index * head_width, head_width
    )
    value_bias = lax.dynamic_slice_in_dim(
        params_all, 3 * model_width + tensor_index * head_width, head_width
    )
    heads = head_width // head_size
    plain, turned, hot, back = attention_tables(rel_tables.astype(NARROW), grid_side)
    token_rows = tokens.reshape(local_rows, model_width).astype(SINGLE)
    normed_one, scaled_one, inverse_one = normalize(token_rows, segment(0), segment(1))
    qkv_bias = jnp.stack([query_bias, jnp.zeros((head_width,), SINGLE), value_bias])
    gathered_one, qkv_rows = gather_rows(
        normed_one.astype(NARROW),
        (qkv_full, qkv_bias[:, None]),
        (jax.ShapeDtypeStruct((3, seq_length, head_width), NARROW),),
        project_rows, tensor_count, 2, "gather_project",
    )
    context_rows, bias_wide, logsums = attend_forward(
        qkv_rows, turned, hot, heads, head_size, grid_side
    )
    attn_sum = scatter_rows(context_rows[None], out_full[None], False, tensor_count, 3, "scatter_out")
    mid_rows = token_rows + (attn_sum + segment(4))
    normed_two, scaled_two, inverse_two = normalize(mid_rows, segment(5), segment(6))
    normed_two_low = normed_two.astype(NARROW)
    expand_bias = lax.dynamic_slice_in_dim(
        params_all, 8 * model_width + tensor_index * hidden_width, hidden_width
    )
    gathered_two, hidden_low, hidden_slope = gather_rows(
        normed_two_low,
        (expand_full, expand_bias[None]),
        (
            jax.ShapeDtypeStruct((seq_length, hidden_width), NARROW),
            jax.ShapeDtypeStruct((seq_length, hidden_width), SINGLE),
        ),
        expand_rows, tensor_count, 4, "gather_expand",
    )
    grad_block = cotangent_rows.astype(SINGLE)
    grad_reduce_bias = jnp.sum(grad_block, axis=0)
    mlp_part = jnp.dot(hidden_low, reduce_full, preferred_element_type=SINGLE).astype(NARROW)
    shard_rows, mlp_part = lax.optimization_barrier((output_grads, mlp_part))
    mlp_sum = lax.psum_scatter(mlp_part, "tensor", scatter_dimension=0, tiled=True)
    part_hidden = contract_cols(shard_rows, reduce_full)
    grad_hidden = part_hidden
    grad_hidden, grad_reduce = (grad_hidden, contract_rows(shard_rows, hidden_low))
    grad_pre = (grad_hidden * hidden_slope).astype(NARROW)
    grad_expand = contract_rows(gathered_two, grad_pre)
    grad_expand_bias = jnp.sum(grad_pre, axis=0, dtype=SINGLE)
    expand_bias_full = lax.dynamic_update_slice_in_dim(
        jnp.zeros((hidden_width * tensor_count,), SINGLE),
        grad_expand_bias,
        tensor_index * hidden_width,
        0,
    )
    grad_reduce, grad_expand = (grad_reduce.astype(NARROW), grad_expand.astype(NARROW))
    grad_pre, grad_reduce, grad_expand = lax.optimization_barrier(
        (grad_pre, grad_reduce, grad_expand)
    )
    reduce_sum = lax.psum_scatter(grad_reduce, "dp", scatter_dimension=0, tiled=True)
    expand_sum = lax.psum_scatter(grad_expand, "dp", scatter_dimension=0, tiled=True)
    grad_normed_two = scatter_rows(
        grad_pre[None], expand_full[None], True, tensor_count, 5, "scatter_expand"
    )
    grad_mid_norm, grad_gain_two, grad_shift_two = normalize_back(
        grad_normed_two, scaled_two, inverse_two, segment(5)
    )
    grad_mid = grad_block + grad_mid_norm
    grad_attn_low = grad_mid.astype(NARROW)
    late_rows = lax.optimization_barrier((mid_rows, grad_normed_two))[0]
    block_rows = late_rows + (mlp_sum.astype(SINGLE) + segment(7))
    block_out = block_rows.astype(NARROW).reshape(tokens.shape)
    grad_attn_low, block_out = lax.optimization_barrier((grad_attn_low, block_out))
    grad_out_bias = jnp.sum(grad_attn_low, axis=0, dtype=SINGLE)
    shard_rows, grad_context = gather_rows(
        grad_attn_low,
        (out_full,),
        (jax.ShapeDtypeStruct((seq_length, head_width), NARROW),),
        context_grad_rows, tensor_count, 6, "gather_context",
    )
    grad_out = contract_rows(shard_rows, context_rows).astype(NARROW)
    grad_context, reduce_sum = lax.optimization_barrier((grad_context, reduce_sum))
    grad_qkv_rows, grad_tables = attend_backward(
        qkv_rows, grad_context, bias_wide, logsums, plain, hot, back,
        heads, head_size, grid_side,
    )
    grad_query_bias = jnp.sum(grad_qkv_rows[0], axis=0, dtype=SINGLE)
    grad_value_bias = jnp.sum(grad_qkv_rows[2], axis=0, dtype=SINGLE)
    grad_qkv = jnp.concatenate(
        [contract_rows(gathered_one, grad_qkv_rows[part]).astype(NARROW) for part in range(3)]
        + [grad_out],
        axis=1,
    )
    grad_qkv_rows, grad_qkv, expand_sum = lax.optimization_barrier(
        (grad_qkv_rows, grad_qkv, expand_sum)
    )
    grad_normed_one = scatter_rows(
        grad_qkv_rows, qkv_full, True, tensor_count, 7, "scatter_qkv"
    )
    grad_token_norm, grad_gain_one, grad_shift_one = normalize_back(
        grad_normed_one, scaled_one, inverse_one, segment(0)
    )
    token_grad = (grad_mid + grad_token_norm).reshape(tokens.shape)
    rel_own = grad_tables.reshape(2, 64, head_size)[:, : rel_tables.shape[1]]
    width_zeros = jnp.zeros((model_width,), SINGLE)
    grad_small = jnp.concatenate(
        [
            grad_gain_one,
            grad_shift_one,
            lax.dynamic_update_slice_in_dim(
                width_zeros, grad_query_bias, tensor_index * head_width, 0
            ),
            lax.dynamic_update_slice_in_dim(
                width_zeros, grad_value_bias, tensor_index * head_width, 0
            ),
            grad_out_bias,
            grad_gain_two,
            grad_shift_two,
            grad_reduce_bias,
            expand_bias_full,
        ]
    )
    devices = lax.axis_size("dp") * tensor_count
    rel_flat = rel_own.reshape(-1)
    rel_piece = -(-rel_flat.shape[0] // devices)
    rel_flat = jnp.pad(rel_flat, (0, rel_piece * devices - rel_flat.shape[0]))
    packed = jnp.concatenate(
        [grad_small.reshape(devices, piece), rel_flat.reshape(devices, rel_piece)], axis=1
    )
    own_sum, rel_grad = small_sum(jax.vmap(as_tiles)(packed), outer, tensor_count, 1)
    gains_grad = own_sum.reshape(-1)[:piece]
    rel_grad = rel_grad.reshape(devices, TILE)[:, piece : piece + rel_piece].reshape(-1)
    rel_grad = rel_grad[: rel_tables.size].reshape(rel_tables.shape)
    heads_sum = lax.psum_scatter(grad_qkv, "dp", scatter_dimension=0, tiled=True).astype(SINGLE)
    qkv_grad = heads_sum[:, : 3 * head_width].reshape(-1, 3, head_width).transpose(1, 0, 2)
    out_grad = heads_sum[:, 3 * head_width :].T
    expand_grad, reduce_grad = (expand_sum.astype(SINGLE), reduce_sum.astype(SINGLE).T)
    reduce_moment = lax.optimization_barrier((reduce_moment, grad_normed_two))[0]
    expand_moment = lax.optimization_barrier((expand_moment, grad_tables))[0]
    out_moment = lax.optimization_barrier((out_moment, grad_normed_one))[0]
    new_qkv, moment_qkv, average_qkv = advance(
        qkv_weight, qkv_moment, qkv_average, qkv_grad, RATE_MAIN
    )
    new_out, moment_out, average_out = advance(
        out_weight, out_moment, out_average, out_grad, RATE_MAIN
    )
    new_expand, moment_expand, average_expand = advance(
        expand_weight, expand_moment, expand_average, expand_grad, RATE_MAIN
    )
    new_reduce, moment_reduce, average_reduce = advance(
        reduce_weight, reduce_moment, reduce_average, reduce_grad, RATE_MAIN
    )
    new_gains, moment_gains, average_gains = advance(
        gains_biases, gains_moment, gains_average, gains_grad, RATE_MAIN
    )
    new_rel, moment_rel, average_rel = advance(
        rel_tables, rel_moment, rel_average, rel_grad, RATE_TABLES
    )
    return (
        block_out,
        token_grad,
        qkv_grad,
        out_grad,
        expand_grad,
        reduce_grad,
        gains_grad,
        rel_grad,
        new_qkv,
        new_out,
        new_expand,
        new_reduce,
        new_gains,
        new_rel,
        moment_qkv,
        moment_out,
        moment_expand,
        moment_reduce,
        moment_gains,
        moment_rel,
        average_qkv,
        average_out,
        average_expand,
        average_reduce,
        average_gains,
        average_rel,
    )


def solution(mesh):
    placed = (
        P("tensor", "dp", None),
        P("tensor", "dp", None),
        P(None, "dp", "tensor"),
        P("tensor", "dp"),
        P("dp", "tensor"),
        P("tensor", "dp"),
        P(("dp", "tensor")),
        P(),
        P(None, "dp", "tensor"),
        P("tensor", "dp"),
        P("dp", "tensor"),
        P("tensor", "dp"),
        P(("dp", "tensor")),
        P(),
        P(None, "dp", "tensor"),
        P("tensor", "dp"),
        P("dp", "tensor"),
        P("tensor", "dp"),
        P(("dp", "tensor")),
        P(),
    )
    return jax.shard_map(
        local,
        mesh=mesh,
        in_specs=placed,
        out_specs=(
            P("tensor", "dp", None),
            P("tensor", "dp", None),
            P(None, "dp", "tensor"),
            P("tensor", "dp"),
            P("dp", "tensor"),
            P("tensor", "dp"),
            P(("dp", "tensor")),
            P(),
            P(None, "dp", "tensor"),
            P("tensor", "dp"),
            P("dp", "tensor"),
            P("tensor", "dp"),
            P(("dp", "tensor")),
            P(),
            P(None, "dp", "tensor"),
            P("tensor", "dp"),
            P("dp", "tensor"),
            P("tensor", "dp"),
            P(("dp", "tensor")),
            P(),
            P(None, "dp", "tensor"),
            P("tensor", "dp"),
            P("dp", "tensor"),
            P("tensor", "dp"),
            P(("dp", "tensor")),
            P(),
        ),
        check_vma=False,
    )
```
